256 devices in a mesh: batch: 2 (over y_lo), space: 64 (over x, y_hi, z), hidden: 2 (over core).
Axes of the slice: x: 4, y: 4 (y_hi: 2, y_lo: 2; y = y_hi * 2 + y_lo), z: 8, core: 2. Of those that a mesh axis runs over, the one named last changes fastest.
Arguments:
- nodes: bfloat16 [2, 8192, 512], P('batch', 'space'), may hold values from -6 to 6
- edges: bfloat16 [2, 65536, 512], P('batch', 'space'), may hold values from -6 to 6
- node_cotangent: bfloat16 [2, 8192, 512], P('batch', 'space'), may hold values from -18 to 18
- edge_cotangent: bfloat16 [2, 65536, 512], P('batch', 'space'), may hold values from -18 to 18
- senders: int32 [65536], P('space'), may hold values from 0 to 255
- receivers: int32 [65536], P('space'), may hold values from 0 to 127
- send_lists: int32 [64, 2, 64], P('space'), may hold values from 0 to 127
- edge_first: bfloat16 [1536, 512], P(None, 'hidden'), may hold values from -0.15625 to 0.15625
- edge_bias: float32 [512], P('hidden'), may hold values from -3 to 3
- edge_second: bfloat16 [512, 512], P('hidden'), may hold values from -0.25 to 0.25
- edge_gain: float32 [512], replicated, may hold values from 0.1 to 1.9
- node_first: bfloat16 [1024, 512], replicated, may hold values from -0.1875 to 0.1875
- node_bias: float32 [512], replicated, may hold values from -3 to 3
- node_second: bfloat16 [512, 512], replicated, may hold values from -0.25 to 0.25
- node_gain: float32 [512], replicated, may hold values from 0.1 to 1.9
Outputs:
- grad_nodes: bfloat16 [2, 8192, 512], P('batch', 'space', 'hidden')
- grad_edges: bfloat16 [2, 65536, 512], P('batch', 'space', 'hidden')
- grad_edge_first: float32 [1536, 512], P(None, 'hidden')
- grad_edge_bias: float32 [512], P('hidden')
- grad_edge_second: float32 [512, 512], P('hidden')
- grad_edge_gain: float32 [512], replicated
- grad_node_first: float32 [1024, 512], replicated
- grad_node_bias: float32 [512], replicated
- grad_node_second: float32 [512, 512], replicated
- grad_node_gain: float32 [512], replicated
The draws below stay inside these ranges and needn't reach their ends.
Inputs may be any that keep to these rules, and one draw needn't show every extreme that they name: `senders`: an entry below 128 is a local node of the edge's patch; 128 + k is row k of the previous patch's list 1, 192 + k row k of the next patch's list 0. `receivers`: local nodes of the edge's patch. `send_lists`: local nodes of the patch; entries may repeat.
All inputs are finite; a program needn't handle non-finite values.
Results may differ from the reference program's by a relative error of at most 0.015.
Values may be sent and summed in bfloat16 or wider, within the bound.
No kernel may reach another device: no remote copies, remote signals or barrier semaphores. Data moves between devices by JAX's collectives and lax.ppermute only.
A program may use at most 128 MiB of HBM per device.

```python
import jax
import jax.numpy as jnp
from jax import lax

D = 512
FF = 512
NODE_DEV = 128
HALO = 64
EDGE_DEV = 1024
TAB = 256
PATCHES = 64
NODES = 8192
EDGES = 65536
SAMPLES = 2


def rising_rows(key, row_count, width):
    first_key = jax.random.fold_in(key, 0)
    ramp = 1.0 + 2.0 * jnp.arange(row_count, dtype=jnp.float32) / row_count
    base = jnp.clip(jax.random.normal(first_key, (SAMPLES, row_count, width), jnp.float32), -6.0, 6.0)
    return base * ramp[None, :, None]


def draw_node_cotangent(key, part):
    return rising_rows(jax.random.fold_in(key, 7), NODES, D).astype(jnp.bfloat16)


def draw_edge_cotangent(key, part):
    return rising_rows(jax.random.fold_in(key, 11), EDGES, D).astype(jnp.bfloat16)


def plant(values, own_key, least, largest):
    spot = [jax.random.randint(jax.random.fold_in(own_key, axis), (), 0, length) for axis, length in enumerate(values.shape)]
    widest = values.shape.index(max(values.shape))
    neighbour = spot[:widest] + [(spot[widest] + 1) % values.shape[widest]] + spot[widest + 1:]
    return values.at[tuple(spot)].set(least).at[tuple(neighbour)].set(largest)


def levels(own_key, dims, cuts, low, top_value):
    level, own = 1.0, jax.random.fold_in(own_key, 6)
    for position, shards_of in cuts:
        steps = jnp.exp(jax.random.uniform(jax.random.fold_in(own, position), (shards_of,), jnp.float32, low / len(cuts), top_value / len(cuts)))
        level = level * jnp.repeat(steps, dims[position] // shards_of).reshape([-1 if axis == position else 1 for axis in range(len(dims))])
    return level


def normal_values(rng, dims, spread, most, pieces=(), held_as=jnp.bfloat16):
    drawn = spread * jax.random.normal(rng, dims, jnp.float32)
    if pieces:
        drawn = drawn * levels(rng, dims, pieces, -0.22, 0.18)
    return jnp.clip(drawn, -most, most).astype(held_as)


def setup_inputs(seed: int = 0) -> dict:
    seeds = jax.random.split(jax.random.key(seed), 16)
    nodes = normal_values(seeds[0], (SAMPLES, NODES, D), 1.0, 6.0, ((0, 2), (1, 64)))
    edges = normal_values(seeds[1], (SAMPLES, EDGES, D), 1.0, 6.0, ((0, 2), (1, 64)))
    node_cotangent = draw_node_cotangent(jax.random.fold_in(seeds[15], 71), 0)
    edge_cotangent = draw_edge_cotangent(jax.random.fold_in(seeds[15], 71), 0)
    senders = plant(jax.random.randint(seeds[4], (EDGES,), 0, TAB), jax.random.fold_in(seeds[4], 1), 0, TAB - 1).astype(jnp.int32)
    receivers = plant(jax.random.randint(seeds[5], (EDGES,), 0, NODE_DEV), jax.random.fold_in(seeds[5], 1), 0, NODE_DEV - 1).astype(jnp.int32)
    send_lists = plant(jax.random.randint(seeds[6], (PATCHES, 2, HALO), 0, NODE_DEV), jax.random.fold_in(seeds[6], 1), 0, NODE_DEV - 1).astype(jnp.int32)
    edge_first = normal_values(seeds[7], (3 * D, FF), (3 * D) ** -0.5, 0.15625, ((1, 2),))
    edge_bias = normal_values(seeds[8], (FF,), 0.5, 3.0, ((0, 2),), jnp.float32)
    edge_second = normal_values(seeds[9], (FF, D), FF ** -0.5, 0.25, ((0, 2),))
    edge_gain = jnp.clip(1.0 + 0.18 * jax.random.normal(seeds[10], (D,), jnp.float32), 0.1, 1.9)
    node_first = normal_values(seeds[11], (2 * D, FF), (2 * D) ** -0.5, 0.1875)
    node_bias = normal_values(seeds[12], (FF,), 0.5, 3.0, (), jnp.float32)
    node_second = normal_values(seeds[13], (FF, D), FF ** -0.5, 0.25)
    node_gain = jnp.clip(1.0 + 0.18 * jax.random.normal(seeds[14], (D,), jnp.float32), 0.1, 1.9)
    return {"nodes": nodes, "edges": edges, "node_cotangent": node_cotangent, "edge_cotangent": edge_cotangent, "senders": senders, "receivers": receivers, "send_lists": send_lists, "edge_first": edge_first, "edge_bias": edge_bias, "edge_second": edge_second, "edge_gain": edge_gain, "node_first": node_first, "node_bias": node_bias, "node_second": node_second, "node_gain": node_gain}


EPS = 1e-05

def matmul(lefthand, righthand):
    return jnp.dot(lefthand, righthand, preferred_element_type=jnp.float32)

def matmul_tn(lefthand, righthand):
    return lax.dot_general(lefthand, righthand, (((0,), (0,)), ((), ())), preferred_element_type=jnp.float32)

def matmul_nt(lefthand, righthand):
    return lax.dot_general(lefthand, righthand, (((1,), (1,)), ((), ())), preferred_element_type=jnp.float32)

def normalize(values):
    centre = values - lax.optimization_barrier(jnp.mean(values, axis=-1, keepdims=True))
    scaled = lax.rsqrt(lax.optimization_barrier(jnp.mean(centre * centre, axis=-1, keepdims=True)) + EPS)
    return (centre * scaled, scaled)

def norm_back(upstream, gain_vec, normed, scaled):
    pulled = upstream * gain_vec
    return scaled * (pulled - lax.optimization_barrier(jnp.mean(pulled, axis=-1, keepdims=True)) - normed * lax.optimization_barrier(jnp.mean(pulled * normed, axis=-1, keepdims=True)))

def silu_slope(values):
    logistic = jax.nn.sigmoid(values)
    return logistic * (1.0 + values * (1.0 - logistic))

def reference(nodes, edges, node_cotangent, edge_cotangent, senders, receivers, send_lists, edge_first, edge_bias, edge_second, edge_gain, node_first, node_bias, node_second, node_gain):
    samples = nodes.shape[0]
    patch_ids = jnp.arange(PATCHES, dtype=jnp.int32)[:, None]
    sample_ids = jnp.arange(samples, dtype=jnp.int32)[:, None]
    node_blocks = nodes.reshape(samples, PATCHES, NODE_DEV, D)
    send_ids = senders.reshape(PATCHES, EDGE_DEV)
    recv_ids = receivers.reshape(PATCHES, EDGE_DEV)
    to_prev = node_blocks[:, patch_ids, send_lists[:, 0, :]]
    to_next = node_blocks[:, patch_ids, send_lists[:, 1, :]]
    table = jnp.concatenate([node_blocks, jnp.roll(to_next, 1, axis=1), jnp.roll(to_prev, -1, axis=1)], axis=2)
    from_sender = table[:, patch_ids, send_ids]
    from_receiver = node_blocks[:, patch_ids, recv_ids]
    edge_blocks = edges.reshape(samples, PATCHES, EDGE_DEV, D)
    edge_input = jnp.concatenate([edge_blocks, from_sender, from_receiver], axis=3).reshape(-1, 3 * D)
    edge_pre = matmul(edge_input, edge_first) + edge_bias
    edge_act = jax.nn.silu(edge_pre).astype(jnp.bfloat16)
    edge_normed, edge_scale = normalize(matmul(edge_act, edge_second))
    message = (edge_gain * edge_normed).astype(jnp.bfloat16)
    flat_recv = (patch_ids * NODE_DEV + recv_ids).reshape(-1)
    segment_ids = (sample_ids * NODES + flat_recv[None, :]).reshape(-1)
    gathered = jax.ops.segment_sum(message.astype(jnp.float32), segment_ids, num_segments=samples * NODES).astype(jnp.bfloat16)
    node_input = jnp.concatenate([nodes.reshape(-1, D), gathered], axis=1)
    node_pre = matmul(node_input, node_first) + node_bias
    node_act = jax.nn.silu(node_pre).astype(jnp.bfloat16)
    node_normed, node_scale = normalize(matmul(node_act, node_second))
    node_upstream = node_cotangent.reshape(-1, D).astype(jnp.float32)
    grad_node_gain = lax.optimization_barrier(jnp.sum(node_upstream * node_normed, axis=0))
    node_dz = norm_back(node_upstream, node_gain, node_normed, node_scale).astype(jnp.bfloat16)
    grad_node_second = matmul_tn(node_act, node_dz)
    node_dh = (matmul_nt(node_dz, node_second) * silu_slope(node_pre)).astype(jnp.bfloat16)
    grad_node_first = matmul_tn(node_input, node_dh)
    grad_node_bias = lax.optimization_barrier(jnp.sum(node_dh.astype(jnp.float32), axis=0))
    node_dx = matmul_nt(node_dh, node_first)
    agg_grad = node_dx[:, D:].astype(jnp.bfloat16)
    edge_upstream = edge_cotangent.reshape(-1, D).astype(jnp.float32)
    message_grad = edge_upstream + agg_grad[segment_ids].astype(jnp.float32)
    grad_edge_gain = lax.optimization_barrier(jnp.sum(message_grad * edge_normed, axis=0))
    edge_dz = norm_back(message_grad, edge_gain, edge_normed, edge_scale).astype(jnp.bfloat16)
    grad_edge_second = matmul_tn(edge_act, edge_dz)
    edge_dh = (matmul_nt(edge_dz, edge_second) * silu_slope(edge_pre)).astype(jnp.bfloat16)
    grad_edge_first = matmul_tn(edge_input, edge_dh)
    grad_edge_bias = lax.optimization_barrier(jnp.sum(edge_dh.astype(jnp.float32), axis=0))
    edge_part = matmul_nt(edge_dh, edge_first[:D])
    grad_edges = (edge_upstream + edge_part).astype(jnp.bfloat16).reshape(samples, EDGES, D)
    send_part = matmul_nt(edge_dh, edge_first[D:2 * D])
    table_ids = (sample_ids * (PATCHES * TAB) + (patch_ids * TAB + send_ids).reshape(-1)[None, :]).reshape(-1)
    table_grad = jax.ops.segment_sum(send_part, table_ids, num_segments=samples * PATCHES * TAB).reshape(samples, PATCHES, TAB, D)
    recv_part = matmul_nt(edge_dh, edge_first[2 * D:])
    recv_grad = jax.ops.segment_sum(recv_part, segment_ids, num_segments=samples * NODES).reshape(samples, PATCHES, NODE_DEV, D)
    own_grad = table_grad[:, :, :NODE_DEV] + recv_grad
    back_prev = jnp.roll(table_grad[:, :, NODE_DEV + HALO:], 1, axis=1)
    back_next = jnp.roll(table_grad[:, :, NODE_DEV:NODE_DEV + HALO], -1, axis=1)
    own_grad = own_grad.at[:, patch_ids, send_lists[:, 0, :]].add(back_prev)
    own_grad = own_grad.at[:, patch_ids, send_lists[:, 1, :]].add(back_next)
    grad_nodes = (node_upstream + node_dx[:, :D] + own_grad.reshape(-1, D)).astype(jnp.bfloat16).reshape(samples, NODES, D)
    return (grad_nodes, grad_edges, grad_edge_first, grad_edge_bias, grad_edge_second, grad_edge_gain, grad_node_first, grad_node_bias, grad_node_second, grad_node_gain)
```

```python
import functools

import jax
import jax.numpy as jnp
from jax import lax
from jax.experimental import pallas as pl
from jax.experimental.pallas import tpu as pltpu
from jax.sharding import PartitionSpec as P

EPS = 1e-05
BF = jnp.bfloat16
F32 = jnp.float32
ALL = ("batch", "space", "hidden")

NX, NY, NZ = 4, 4, 8
VEC = 16


def device_at(x, y, z, core):
    return ((y % 2) * 64 + (x * 2 + y // 2) * 8 + z) * 2 + core


def cube_member(core, a, b, c, i, j, k):
    return device_at(
        (2 * a + i + core) % NX, (2 * b + j + core) % NY, (2 * c + k + core) % NZ, core
    )


CUBE = [(i, j, k) for i in range(2) for j in range(2) for k in range(2)]
REST = [(a, b, c) for a in range(2) for b in range(2) for c in range(4)]
NEAR = [[cube_member(core, *r, *m) for m in CUBE] for core in range(2) for r in REST]
FAR = [[cube_member(core, *r, *m) for r in REST] for core in range(2) for m in CUBE]


def dot(a, b):
    return jnp.dot(a, b, preferred_element_type=F32)


def dot_tn(a, b):
    return lax.dot_general(a, b, (((0,), (0,)), ((), ())), preferred_element_type=F32)


def dot_nt(a, b):
    return lax.dot_general(a, b, (((1,), (1,)), ((), ())), preferred_element_type=F32)


def silu_parts(pre):
    s = 0.5 * jnp.tanh(0.5 * pre) + 0.5
    return pre * s, s * (1.0 + pre * (1.0 - s))


def row_mean(v):
    return jnp.sum(v, axis=1, keepdims=True) * (1.0 / v.shape[1])


def normalize(z):
    centre = z - row_mean(z)
    scale = lax.rsqrt(row_mean(centre * centre) + EPS)
    return centre * scale, scale


def norm_back(g, normed, scale):
    return scale * (g - row_mean(g) - normed * row_mean(g * normed))


def layer_kernel(
    h_ref,
    snd,
    rcv,
    edges,
    ecot,
    nodes,
    ncot,
    halo_p,
    halo_n,
    w1m,
    w1o,
    b1m,
    b1o,
    w2m,
    w2o,
    egain,
    nf,
    nb,
    ns,
    ngain,
    grads,
    gedges,
    gnodes,
    back,
    table,
    tw,
    hot,
    act,
    slope,
    normed,
    scale,
    dz,
    dh,
    msum,
    ndh,
    ndz,
    ndx,
    aggr,
    ginp,
):
    E, D = edges.shape
    N = nodes.shape[0]
    H = w1m.shape[1]
    T = table.shape[0]
    half = D // 2
    own = pl.multiple_of(h_ref[0] * half, half)
    rows = 256
    blocks = E // rows

    def put(at, value):
        value = value.astype(BF)
        n = value.shape[0]
        per = grads.shape[1] - VEC
        done = 0
        while done < n:
            piece, off = divmod(at + done, per)
            take = min(n - done, per - off)
            for side in range(2):
                grads[piece + 4 * side, off : off + take, :] = value[
                    done : done + take, side * 128 : side * 128 + 128
                ]
            done += take

    table[0:N, :] = nodes[...]
    table[N : N + halo_p.shape[0], :] = halo_p[...]
    table[N + halo_p.shape[0] :, :] = halo_n[...]
    for side, w in enumerate((w1m, w1o)):
        cols = slice(side * H, side * H + H)
        tw[0:T, cols] = dot(table[...], w[D : 2 * D, :]).astype(BF)
        tw[T:, cols] = dot(nodes[...], w[2 * D :, :]).astype(BF)
    hot[0:T, :] = (lax.broadcasted_iota(jnp.int32, (T, E), 0) == snd[...]).astype(F32).astype(BF)
    hot[T:, :] = (lax.broadcasted_iota(jnp.int32, (N, E), 0) == rcv[...]).astype(F32).astype(BF)
    bias = jnp.concatenate([b1m[...], b1o[...]], axis=1)
    aggr[...] = jnp.zeros_like(aggr)

    @pl.loop(0, blocks)
    def _(b):
        at = pl.ds(pl.multiple_of(b * rows, rows), rows)
        e = edges[at, :]
        pre = jnp.concatenate([dot(e, w1m[0:D, :]), dot(e, w1o[0:D, :])], axis=1)
        pre = pre + dot_tn(hot[:, at], tw[...]) + bias
        a, sl = silu_parts(pre)
        a = a.astype(BF)
        act[at, :] = a
        slope[at, :] = sl
        z = dot(a[:, 0:H], w2m[...]) + dot(a[:, H:], w2o[...])
        nz, sc = normalize(z)
        normed[at, :] = nz
        scale[at, :] = sc
        message = (egain[...] * nz).astype(BF)
        aggr[...] += dot(hot[T:, at], message)

    agg = aggr[...].astype(BF)
    ginp[:, 0:D] = nodes[...]
    ginp[:, D:] = agg
    npre = dot(ginp[...], nf[...]) + nb[...]
    nact, nslope = silu_parts(npre)
    nact = nact.astype(BF)
    nnorm, nscale = normalize(dot(nact, ns[...]))
    up = ncot[...].astype(F32)
    gain_n = jnp.sum(up * nnorm, axis=0, keepdims=True)
    dzn = norm_back(ngain[...] * up, nnorm, nscale).astype(BF)
    ndz[...] = dzn
    dhn = (dot_nt(dzn, ns[...]) * nslope).astype(BF)
    ndh[...] = dhn
    bias_n = jnp.sum(dhn.astype(F32), axis=0, keepdims=True)
    put(3 * D + 2 * H, dot_tn(ginp[...], ndh[:, pl.ds(own, half)]))
    put(5 * D + 2 * H, dot_tn(nact, ndz[:, pl.ds(own, half)]))
    dxn = dot_nt(dhn, nf[...])
    ndx[...] = dxn[:, 0:D]
    ag = dxn[:, D:].astype(BF)
    msum[...] = jnp.zeros_like(msum)

    @pl.loop(0, blocks)
    def _(b):
        at = pl.ds(pl.multiple_of(b * rows, rows), rows)
        mg = ecot[at, :].astype(F32) + dot_tn(hot[T:, at], ag)
        nz = normed[at, :]
        msum[0:8, :] += jnp.sum((mg * nz).reshape(rows // 8, 8, D), axis=0)
        d = norm_back(egain[...] * mg, nz, scale[at, :]).astype(BF)
        dz[at, :] = d
        g = jnp.concatenate([dot_nt(d, w2m[...]), dot_nt(d, w2o[...])], axis=1)
        g = (g * slope[at, :]).astype(BF)
        dh[at, :] = g
        msum[8:16, :] += jnp.sum(g.astype(F32).reshape(rows // 8, 8, D), axis=0)
        part = dot_nt(g[:, 0:H], w1m[pl.ds(own, half), :]) + dot_nt(
            g[:, H:], w1o[pl.ds(own, half), :]
        )
        gedges[at, :] = (ecot[at, pl.ds(own, half)].astype(F32) + part).astype(BF)

    second = dot_tn(act[:, 0:H], dz[...])
    put(3 * D, second[:, 0:half])
    put(3 * D + H, second[:, half:])
    put(0, dot_tn(edges[...], dh[:, 0:H]))
    u = dot(hot[...], dh[...]).astype(BF)
    put(D, dot_tn(table[...], u[0:T, 0:H]))
    put(2 * D, dot_tn(nodes[...], u[T:, 0:H]))
    at_s = pl.ds(pl.multiple_of(D + own, half), half)
    at_r = pl.ds(pl.multiple_of(2 * D + own, half), half)
    tg = dot_nt(u[0:T, 0:H], w1m[at_s, :]) + dot_nt(u[0:T, H:], w1o[at_s, :])
    rg = dot_nt(u[T:, 0:H], w1m[at_r, :]) + dot_nt(u[T:, H:], w1o[at_r, :])
    gnodes[...] = ncot[:, pl.ds(own, half)].astype(F32) + ndx[:, pl.ds(own, half)] + tg[0:N] + rg
    back[...] = tg[N:, :].astype(BF)

    gain_e = jnp.sum(msum[0:8, :], axis=0, keepdims=True)
    bias_e = jnp.sum(msum[8:16, :], axis=0, keepdims=True)[:, 0:H]
    parts = []
    for v in (bias_e, gain_e, bias_n, gain_n):
        parts += [v[:, i : i + 128] for i in range(0, v.shape[1], 128)]
    parts.append(jnp.zeros((VEC - len(parts), 128), F32))
    vec = jnp.concatenate(parts, axis=0).astype(BF)
    for piece in range(grads.shape[0]):
        grads[piece, grads.shape[1] - VEC :, :] = vec


def run_layer(h, args):
    edges, nodes, w1m = args[2], args[4], args[8]
    E, D = edges.shape
    N = nodes.shape[0]
    H = w1m.shape[1]
    halo = args[6].shape[0]
    T = N + 2 * halo
    total = 3 * D + 2 * H + 3 * D
    per = total * 2 // 8
    vm = pl.BlockSpec(memory_space=pltpu.VMEM)
    return pl.pallas_call(
        layer_kernel,
        out_shape=(
            jax.ShapeDtypeStruct((8, per + VEC, 128), BF),
            jax.ShapeDtypeStruct((E, D // 2), BF),
            jax.ShapeDtypeStruct((N, D // 2), F32),
            jax.ShapeDtypeStruct((2 * halo, D // 2), BF),
        ),
        in_specs=[pl.BlockSpec(memory_space=pltpu.SMEM)] + [vm] * len(args),
        out_specs=(vm, vm, vm, vm),
        scratch_shapes=[
            pltpu.VMEM((T, D), BF),
            pltpu.VMEM((T + N, 2 * H), BF),
            pltpu.VMEM((T + N, E), BF),
            pltpu.VMEM((E, 2 * H), BF),
            pltpu.VMEM((E, 2 * H), F32),
            pltpu.VMEM((E, D), F32),
            pltpu.VMEM((E, 1), F32),
            pltpu.VMEM((E, D), BF),
            pltpu.VMEM((E, 2 * H), BF),
            pltpu.VMEM((16, D), F32),
            pltpu.VMEM((N, D), BF),
            pltpu.VMEM((N, D), BF),
            pltpu.VMEM((N, D), F32),
            pltpu.VMEM((N, D), F32),
            pltpu.VMEM((N, 2 * D), BF),
        ],
        compiler_params=pltpu.CompilerParams(vmem_limit_bytes=44 * 1024 * 1024),
        cost_estimate=pl.CostEstimate(
            flops=6_000_000_000, bytes_accessed=12_000_000, transcendentals=1_000_000
        ),
        name="layer",
    )(h, *args)


def all_pieces(value, groups):
    return lax.all_to_all(value, ALL, 0, 0, axis_index_groups=groups, tiled=True)


def summed(pieces):
    return jnp.sum(pieces.astype(F32), axis=0)


def on_device(
    nodes,
    edges,
    node_cotangent,
    edge_cotangent,
    senders,
    receivers,
    send_lists,
    edge_first,
    edge_bias,
    edge_second,
    edge_gain,
    node_first,
    node_bias,
    node_second,
    node_gain,
):
    h = lax.axis_index("hidden").astype(jnp.int32)
    swap = [(0, 1), (1, 0)]
    count = lax.axis_size("space")
    onward = [(i, (i + 1) % count) for i in range(count)]
    backward = [((i + 1) % count, i) for i in range(count)]
    rows = nodes[0]
    N, D = rows.shape
    H = edge_first.shape[1]
    half = D // 2
    halo = send_lists.shape[2]

    first_other = lax.ppermute(edge_first, "hidden", swap)
    second_other = lax.ppermute(edge_second, "hidden", swap)
    bias_row = edge_bias[None]
    bias_other = lax.ppermute(bias_row, "hidden", swap)
    listed = send_lists[0].reshape(-1)
    picker = (listed[:, None] == jnp.arange(N, dtype=jnp.int32)[None, :]).astype(BF)
    outgoing = dot(picker, rows).astype(BF)
    from_prev = lax.ppermute(outgoing[halo:], "space", onward)
    from_next = lax.ppermute(outgoing[:halo], "space", backward)

    grads, gedges, gnodes, back = run_layer(
        h[None],
        (
            senders[None],
            receivers[None],
            edges[0],
            edge_cotangent[0],
            rows,
            node_cotangent[0],
            from_prev,
            from_next,
            edge_first,
            first_other,
            bias_row,
            bias_other,
            edge_second,
            second_other,
            edge_gain[None],
            node_first,
            node_bias[None],
            node_second,
            node_gain[None],
        ),
    )
    to_prev = lax.ppermute(back[:halo], "space", backward)
    to_next = lax.ppermute(back[halo:], "space", onward)

    got = summed(all_pieces(grads, NEAR)).astype(BF)
    body, vec = got[:-VEC], got[-VEC:]
    far = len(FAR[0])
    pieces = jnp.concatenate(
        [
            body.reshape(far, -1, 128),
            jnp.broadcast_to(vec[None], (far, VEC, 128)),
        ],
        axis=1,
    )
    got = summed(all_pieces(pieces, FAR))
    vec = got[-VEC:].reshape(-1)
    part = got[:-VEC].astype(BF)
    part = all_pieces(jnp.broadcast_to(part[None], (far, *part.shape)), FAR)
    part = part.reshape(-1, 128)
    near = len(NEAR[0])
    full = all_pieces(jnp.broadcast_to(part[None], (near, *part.shape)), NEAR)
    full = full.reshape(2, -1, 128)

    arriving = jnp.concatenate([to_next, to_prev], axis=0)
    placer = (jnp.arange(N, dtype=jnp.int32)[:, None] == listed[None, :]).astype(BF)
    grad_nodes = (gnodes + dot(placer, arriving)).astype(BF)[None]

    mine = full[:, 3 * D + 2 * H :]
    other = lax.ppermute(mine, "hidden", swap)

    def wide(v):
        return jnp.concatenate([v[0], v[1]], axis=1).astype(F32)

    edge_first_grad = wide(full[:, : 3 * D])
    edge_second_grad = jnp.concatenate(
        [wide(full[:, 3 * D : 3 * D + H]), wide(full[:, 3 * D + H : 3 * D + 2 * H])], axis=1
    )
    low = jnp.where(h == 0, mine, other)
    high = jnp.where(h == 0, other, mine)
    node_grad = jnp.concatenate([wide(low), wide(high)], axis=1)
    return (
        grad_nodes,
        gedges[None],
        edge_first_grad,
        vec[:H],
        edge_second_grad,
        vec[H : H + D],
        node_grad[: 2 * D],
        vec[H + D : H + 2 * D],
        node_grad[2 * D :],
        vec[H + 2 * D : H + 3 * D],
    )


def solution(mesh):
    placed = (
        P("batch", "space", None),
        P("batch", "space", None),
        P("batch", "space", None),
        P("batch", "space", None),
        P("space"),
        P("space"),
        P("space", None, None),
        P(None, "hidden"),
        P("hidden"),
        P("hidden", None),
        P(),
        P(),
        P(),
        P(),
        P(),
    )
    return jax.shard_map(
        on_device,
        mesh=mesh,
        in_specs=placed,
        out_specs=(
            P("batch", "space", "hidden"),
            P("batch", "space", "hidden"),
            P(None, "hidden"),
            P("hidden"),
            P("hidden", None),
            P(),
            P(),
            P(),
            P(),
            P(),
        ),
        check_vma=False,
    )
```

```python
import jax
import jax.numpy as jnp
from jax import lax
from jax.experimental import pallas as pl
from jax.experimental.pallas import tpu as pltpu
from jax.sharding import PartitionSpec as P


EPS = 1e-05
BF = jnp.bfloat16
F32 = jnp.float32
ALL = ("batch", "space", "hidden")

NX, NY, NZ = 4, 4, 8
GROUP = 32
PIECE = 224
EXTRA = 8


def device_at(x, y, z, core):
    return ((y % 2) * 64 + (x * 2 + y // 2) * 8 + z) * 2 + core


def place_of(device):
    core, rest = device % 2, device // 2
    b, space = rest // 64, rest % 64
    return space // 16, (space // 8) % 2 * 2 + b, space % 8, core


PLANES = [
    [device_at(x, y, 2 * c + k, core) for x in range(NX) for y in range(NY) for k in range(2)]
    for core in range(2)
    for c in range(NZ // 2)
]


def across_z(bit):
    pairs = []
    for device in range(2 * NX * NY * NZ):
        x, y, z, core = place_of(device)
        pairs.append((device, device_at(x, y, z ^ bit, core)))
    return pairs


def dot(a, b):
    return jnp.dot(a, b, preferred_element_type=F32)


def dot_tn(a, b):
    return lax.dot_general(a, b, (((0,), (0,)), ((), ())), preferred_element_type=F32)


def dot_nt(a, b):
    return lax.dot_general(a, b, (((1,), (1,)), ((), ())), preferred_element_type=F32)


def silu_parts(pre):
    s = 0.5 * jnp.tanh(0.5 * pre) + 0.5
    return pre * s, s * (1.0 + pre * (1.0 - s))


def row_mean(v):
    return jnp.sum(v, axis=1, keepdims=True) * (1.0 / v.shape[1])


def normalize(z):
    centre = z - row_mean(z)
    scale = lax.rsqrt(row_mean(centre * centre) + EPS)
    return centre * scale, scale


def norm_back(g, normed, scale):
    return scale * (g - row_mean(g) - normed * row_mean(g * normed))


def in_hbm(*arrays):
    return tuple(pltpu.with_memory_space_constraint(a, pltpu.HBM) for a in arrays)


def own_columns(width):
    return pl.multiple_of(lax.axis_index("hidden") * width, width)


def copies(pairs, sems, first):
    return [pltpu.make_async_copy(a, b, sems.at[first + i]) for i, (a, b) in enumerate(pairs)]


def pick_kernel(lists, nodes, first, second, lists_v, nodes_v, sems):
    moves = copies([(lists, lists_v), (nodes, nodes_v)], sems, 0)
    for m in moves:
        m.start()
    for m in moves:
        m.wait()
    N, K = nodes_v.shape[0], lists_v.shape[1]
    for i, out in enumerate((first, second)):
        hot = lax.broadcasted_iota(jnp.int32, (N, K), 0) == lists_v[i : i + 1, :]
        out[...] = dot_tn(hot.astype(F32).astype(BF), nodes_v[...]).astype(BF)


def pick(lists, nodes):
    hbm = pl.BlockSpec(memory_space=pltpu.HBM)
    vm = pl.BlockSpec(memory_space=pltpu.VMEM)
    out = jax.ShapeDtypeStruct((lists.shape[1], nodes.shape[1]), BF)
    return pl.pallas_call(
        pick_kernel,
        out_shape=(out, out),
        in_specs=[hbm, hbm],
        out_specs=(vm, vm),
        scratch_shapes=[
            pltpu.VMEM(lists.shape, jnp.int32),
            pltpu.VMEM(nodes.shape, BF),
            pltpu.SemaphoreType.DMA((2,)),
        ],
        compiler_params=pltpu.CompilerParams(vmem_limit_bytes=4 * 1024 * 1024),
        cost_estimate=pl.CostEstimate(flops=200_000_000, bytes_accessed=400_000, transcendentals=0),
        name="pick",
    )(*in_hbm(lists, nodes))


LOADED = 14


def layer_kernel(*refs):
    sources = refs[:LOADED]
    halo_p, halo_n, w1o, b1o, w2o = refs[LOADED : LOADED + 5]
    grads, dh, u, ndx = refs[LOADED + 5 : LOADED + 9]
    loaded = refs[LOADED + 9 : 2 * LOADED + 9]
    (table, tw, hot, act, slope, normed, scale, dz, msum, ndh, ndz, aggr, ginp, sems) = refs[
        2 * LOADED + 9 :
    ]
    snd, rcv, nodes, w1m, b1m, edges, w2m, egain, nf, nb, ns, ngain, ncot, ecot = loaded
    moves = copies(list(zip(sources, loaded)), sems, 0)
    for m in moves:
        m.start()
    E, D = edges.shape
    N = nodes.shape[0]
    H = w1m.shape[1]
    T = table.shape[0]
    half = D // 2
    own = own_columns(half)
    rows = 256
    blocks = E // rows
    side_rows = GROUP * PIECE // 2
    split = (3 * D + 2 * H) // PIECE

    def put(at, value):
        value = value.astype(BF)
        n = value.shape[0]
        done = 0
        while done < n:
            q, off = divmod(at + done, PIECE)
            take = min(n - done, PIECE - off)
            for side in range(2):
                if q < split:
                    piece = q + split * side
                else:
                    piece = 2 * split + (q - split) + (side_rows // PIECE - split) * side
                grads[piece, off : off + take, :] = value[
                    done : done + take, side * 128 : side * 128 + 128
                ]
            done += take

    for m in moves[0:2]:
        m.wait()
    hot[0:T, :] = (lax.broadcasted_iota(jnp.int32, (T, E), 0) == snd[...]).astype(F32).astype(BF)
    hot[T:, :] = (lax.broadcasted_iota(jnp.int32, (N, E), 0) == rcv[...]).astype(F32).astype(BF)
    for m in moves[2:5]:
        m.wait()
    table[0:N, :] = nodes[...]
    table[N : N + halo_p.shape[0], :] = halo_p[...]
    table[N + halo_p.shape[0] :, :] = halo_n[...]
    for side, w in enumerate((w1m, w1o)):
        cols = slice(side * H, side * H + H)
        tw[0:T, cols] = dot(table[...], w[D : 2 * D, :]).astype(BF)
        tw[T:, cols] = dot(nodes[...], w[2 * D :, :]).astype(BF)
    bias = jnp.concatenate([b1m[...], b1o[...]], axis=1)
    aggr[...] = jnp.zeros_like(aggr)
    for m in moves[5:8]:
        m.wait()

    @pl.loop(0, blocks)
    def _(b):
        at = pl.ds(pl.multiple_of(b * rows, rows), rows)
        e = edges[at, :]
        pre = jnp.concatenate([dot(e, w1m[0:D, :]), dot(e, w1o[0:D, :])], axis=1)
        pre = pre + dot_tn(hot[:, at], tw[...]) + bias
        a, sl = silu_parts(pre)
        a = a.astype(BF)
        act[at, :] = a
        slope[at, :] = sl
        z = dot(a[:, 0:H], w2m[...]) + dot(a[:, H:], w2o[...])
        nz, sc = normalize(z)
        normed[at, :] = nz
        scale[at, :] = sc
        message = (egain[...] * nz).astype(BF)
        aggr[...] += dot(hot[T:, at], message)

    for m in moves[8:]:
        m.wait()
    agg = aggr[...].astype(BF)
    ginp[:, 0:D] = nodes[...]
    ginp[:, D:] = agg
    npre = dot(ginp[...], nf[...]) + nb[...]
    nact, nslope = silu_parts(npre)
    nact = nact.astype(BF)
    nnorm, nscale = normalize(dot(nact, ns[...]))
    up = ncot[...].astype(F32)
    gain_n = jnp.sum(up * nnorm, axis=0, keepdims=True)
    dzn = norm_back(ngain[...] * up, nnorm, nscale).astype(BF)
    ndz[...] = dzn
    dhn = (dot_nt(dzn, ns[...]) * nslope).astype(BF)
    ndh[...] = dhn
    bias_n = jnp.sum(dhn.astype(F32), axis=0, keepdims=True)
    put(3 * D + 2 * H, dot_tn(ginp[...], ndh[:, pl.ds(own, half)]))
    put(5 * D + 2 * H, dot_tn(nact, ndz[:, pl.ds(own, half)]))
    dxn = dot_nt(dhn, nf[...])
    ndx[...] = dxn[:, 0:D]
    ag = dxn[:, D:].astype(BF)
    msum[...] = jnp.zeros_like(msum)

    @pl.loop(0, blocks)
    def _(b):
        at = pl.ds(pl.multiple_of(b * rows, rows), rows)
        mg = ecot[at, :].astype(F32) + dot_tn(hot[T:, at], ag)
        nz = normed[at, :]
        msum[0:8, :] += jnp.sum((mg * nz).reshape(rows // 8, 8, D), axis=0)
        d = norm_back(egain[...] * mg, nz, scale[at, :]).astype(BF)
        dz[at, :] = d
        g = jnp.concatenate([dot_nt(d, w2m[...]), dot_nt(d, w2o[...])], axis=1)
        g = (g * slope[at, :]).astype(BF)
        dh[at, :] = g
        msum[8:16, :] += jnp.sum(g.astype(F32).reshape(rows // 8, 8, D), axis=0)

    second = dot_tn(act[:, 0:H], dz[...])
    put(3 * D, second[:, 0:half])
    put(3 * D + H, second[:, half:])
    put(0, dot_tn(edges[...], dh[:, 0:H]))
    u[...] = dot(hot[...], dh[...]).astype(BF)
    put(D, dot_tn(table[...], u[0:T, 0:H]))
    put(2 * D, dot_tn(nodes[...], u[T:, 0:H]))

    gain_e = jnp.sum(msum[0:8, :], axis=0, keepdims=True)
    bias_e = jnp.sum(msum[8:16, :], axis=0, keepdims=True)[:, 0:H]
    parts = []
    for v in (bias_e, gain_e, bias_n, gain_n):
        parts += [v[:, i : i + 128] for i in range(0, v.shape[1], 128)]
    zero = jnp.zeros((2 * EXTRA - len(parts), 128), F32)
    vec = jnp.concatenate(parts + [zero], axis=0).astype(BF)
    for piece in range(GROUP):
        if piece < 2:
            grads[piece, PIECE:, :] = vec[piece * EXTRA : piece * EXTRA + EXTRA]
        else:
            grads[piece, PIECE:, :] = jnp.zeros((EXTRA, 128), BF)


def run_layer(params, arrived):
    N, D = params[2].shape
    H = params[3].shape[1]
    E = params[5].shape[0]
    T = N + 2 * arrived[0].shape[0]
    hbm = pl.BlockSpec(memory_space=pltpu.HBM)
    vm = pl.BlockSpec(memory_space=pltpu.VMEM)
    return pl.pallas_call(
        layer_kernel,
        out_shape=(
            jax.ShapeDtypeStruct((GROUP, PIECE + EXTRA, 128), BF),
            jax.ShapeDtypeStruct((E, 2 * H), BF),
            jax.ShapeDtypeStruct((T + N, 2 * H), BF),
            jax.ShapeDtypeStruct((N, D), F32),
        ),
        in_specs=[hbm] * LOADED + [vm] * len(arrived),
        out_specs=(vm, vm, vm, vm),
        scratch_shapes=[pltpu.VMEM(p.shape, p.dtype) for p in params]
        + [
            pltpu.VMEM((T, D), BF),
            pltpu.VMEM((T + N, 2 * H), BF),
            pltpu.VMEM((T + N, E), BF),
            pltpu.VMEM((E, 2 * H), BF),
            pltpu.VMEM((E, 2 * H), F32),
            pltpu.VMEM((E, D), F32),
            pltpu.VMEM((E, 1), F32),
            pltpu.VMEM((E, D), BF),
            pltpu.VMEM((16, D), F32),
            pltpu.VMEM((N, D), BF),
            pltpu.VMEM((N, D), BF),
            pltpu.VMEM((N, D), F32),
            pltpu.VMEM((N, 2 * D), BF),
            pltpu.SemaphoreType.DMA((LOADED,)),
        ],
        compiler_params=pltpu.CompilerParams(vmem_limit_bytes=40 * 1024 * 1024),
        cost_estimate=pl.CostEstimate(
            flops=6_000_000_000, bytes_accessed=12_000_000, transcendentals=1_000_000
        ),
        name="layer",
    )(*in_hbm(*params), *arrived)


def inputs_kernel(
    w1m, ecot, ncot, w1o, dh, u, ndx, gedges, gnodes, to_prev, to_next, w1m_v, ecot_v, ncot_v, out, sems
):
    D = ncot.shape[1]
    H = w1m.shape[1]
    N = ncot.shape[0]
    T = u.shape[0] - N
    half = D // 2
    own = own_columns(half)
    K = to_prev.shape[0]
    moves = copies(
        [
            (w1m, w1m_v),
            (ecot.at[:, pl.ds(own, half)], ecot_v),
            (ncot.at[:, pl.ds(own, half)], ncot_v),
        ],
        sems,
        0,
    )
    for m in moves:
        m.start()
    moves[0].wait()
    moves[2].wait()
    at_s = pl.ds(pl.multiple_of(D + own, half), half)
    at_r = pl.ds(pl.multiple_of(2 * D + own, half), half)
    tg = dot_nt(u[0:T, 0:H], w1m_v[at_s, :]) + dot_nt(u[0:T, H:], w1o[at_s, :])
    rg = dot_nt(u[T:, 0:H], w1m_v[at_r, :]) + dot_nt(u[T:, H:], w1o[at_r, :])
    to_prev[...] = tg[N : N + K, :].astype(BF)
    to_next[...] = tg[N + K :, :].astype(BF)
    gnodes[...] = ncot_v[...].astype(F32) + ndx[:, pl.ds(own, half)] + tg[0:N] + rg
    moves[1].wait()
    part = dot_nt(dh[:, 0:H], w1m_v[pl.ds(own, half), :]) + dot_nt(
        dh[:, H:], w1o[pl.ds(own, half), :]
    )
    out[...] = (ecot_v[...].astype(F32) + part).astype(BF)
    last = pltpu.make_async_copy(out, gedges, sems.at[3])
    last.start()
    last.wait()


def run_inputs(w1m, ecot, ncot, w1o, dh, u, ndx, halo):
    N, D = ncot.shape
    E = ecot.shape[0]
    half = D // 2
    hbm = pl.BlockSpec(memory_space=pltpu.HBM)
    vm = pl.BlockSpec(memory_space=pltpu.VMEM)
    sent = jax.ShapeDtypeStruct((halo, half), BF)
    return pl.pallas_call(
        inputs_kernel,
        out_shape=(
            jax.ShapeDtypeStruct((E, half), BF),
            jax.ShapeDtypeStruct((N, half), F32),
            sent,
            sent,
        ),
        in_specs=[hbm, hbm, hbm, vm, vm, vm, vm],
        out_specs=(hbm, vm, vm, vm),
        scratch_shapes=[
            pltpu.VMEM(w1m.shape, BF),
            pltpu.VMEM((E, half), BF),
            pltpu.VMEM((N, half), BF),
            pltpu.VMEM((E, half), BF),
            pltpu.SemaphoreType.DMA((4,)),
        ],
        compiler_params=pltpu.CompilerParams(vmem_limit_bytes=12 * 1024 * 1024),
        cost_estimate=pl.CostEstimate(
            flops=700_000_000, bytes_accessed=3_000_000, transcendentals=0
        ),
        name="inputs",
    )(*in_hbm(w1m, ecot, ncot), w1o, dh, u, ndx)


def node_kernel(lists, gnodes, first, second, out, lists_v, sems):
    move = pltpu.make_async_copy(lists, lists_v, sems.at[0])
    move.start()
    move.wait()
    N, K = gnodes.shape[0], first.shape[0]
    total = gnodes[...]
    for i, value in enumerate((first, second)):
        hot = lax.broadcasted_iota(jnp.int32, (N, K), 0) == lists_v[i : i + 1, :]
        total = total + dot(hot.astype(F32).astype(BF), value[...])
    out[...] = total.astype(BF)


def run_node(lists, gnodes, first, second):
    hbm = pl.BlockSpec(memory_space=pltpu.HBM)
    vm = pl.BlockSpec(memory_space=pltpu.VMEM)
    return pl.pallas_call(
        node_kernel,
        out_shape=jax.ShapeDtypeStruct(gnodes.shape, BF),
        in_specs=[hbm, vm, vm, vm],
        out_specs=vm,
        scratch_shapes=[pltpu.VMEM(lists.shape, jnp.int32), pltpu.SemaphoreType.DMA((1,))],
        compiler_params=pltpu.CompilerParams(vmem_limit_bytes=4 * 1024 * 1024),
        cost_estimate=pl.CostEstimate(flops=100_000_000, bytes_accessed=300_000, transcendentals=0),
        name="node_gradient",
    )(*in_hbm(lists), gnodes, first, second)


def edge_out_kernel(full, first, second, v0, v1, v2, v3, first_v, second_v, sems):
    D3, _ = first.shape
    H = second.shape[0]
    half = second.shape[1] // 2
    split = (D3 + 2 * H) // PIECE
    last = GROUP // 2 - split

    def fetch(at, count, put):
        done = 0
        while done < count:
            q, off = divmod(at + done, PIECE)
            take = min(count - done, PIECE - off)
            for side in range(2):
                if q < split:
                    piece = q + split * side
                else:
                    piece = 2 * split + (q - split) + last * side
                put(done, take, side, full[piece, off : off + take, :].astype(F32))
            done += take

    def put_first(done, take, side, value):
        first_v[done : done + take, side * 128 : side * 128 + 128] = value

    fetch(0, D3, put_first)
    moves = copies([(first_v, first), (second_v, second)], sems, 0)
    moves[0].start()
    for part in range(2):

        def put_second(done, take, side, value):
            at = part * half + side * 128
            second_v[done : done + take, at : at + 128] = value

        fetch(D3 + part * H, H, put_second)
    moves[1].start()
    row = 0
    for out in (v0, v1, v2, v3):
        for at in range(0, out.shape[1], 128):
            piece, off = divmod(row, EXTRA)
            tile = full[piece, PIECE:, :].astype(F32)
            out[:, at : at + 128] = tile[off : off + 1, :]
            row += 1
    for m in moves:
        m.wait()


def run_edge_out(full, D, H):
    hbm = pl.BlockSpec(memory_space=pltpu.HBM)
    vm = pl.BlockSpec(memory_space=pltpu.VMEM)
    shapes = [(3 * D, H), (H, D)]
    outs = shapes + [(1, H), (1, D), (1, D), (1, D)]
    return pl.pallas_call(
        edge_out_kernel,
        out_shape=tuple(jax.ShapeDtypeStruct(s, F32) for s in outs),
        in_specs=[vm],
        out_specs=(hbm, hbm, vm, vm, vm, vm),
        scratch_shapes=[pltpu.VMEM(s, F32) for s in shapes] + [pltpu.SemaphoreType.DMA((2,))],
        compiler_params=pltpu.CompilerParams(vmem_limit_bytes=12 * 1024 * 1024),
        cost_estimate=pl.CostEstimate(flops=1_000_000, bytes_accessed=3_000_000, transcendentals=0),
        name="edge_out",
    )(full)


def node_out_kernel(mine, other, first, second, first_v, second_v, sems):
    D2, D = first.shape
    half = D // 2
    mine_at = own_columns(half)
    other_at = pl.multiple_of(half - mine_at, half)
    skip = (3 * D + D2 // 2) % PIECE
    last = mine.shape[0] // 2
    moves = copies([(first_v, first), (second_v, second)], sems, 0)
    for base, count, out, move in ((0, D2, first_v, moves[0]), (D2, D, second_v, moves[1])):
        for src, col in ((mine, mine_at), (other, other_at)):
            done = 0
            while done < count:
                q, off = divmod(skip + base + done, PIECE)
                take = min(count - done, PIECE - off)
                for side in range(2):
                    at = pl.ds(pl.multiple_of(col + side * 128, 128), 128)
                    out[done : done + take, at] = src[q + last * side, off : off + take, :].astype(
                        F32
                    )
                done += take
        move.start()
    for m in moves:
        m.wait()


def run_node_out(mine, other, D):
    hbm = pl.BlockSpec(memory_space=pltpu.HBM)
    vm = pl.BlockSpec(memory_space=pltpu.VMEM)
    shapes = [(2 * D, D), (D, D)]
    return pl.pallas_call(
        node_out_kernel,
        out_shape=tuple(jax.ShapeDtypeStruct(s, F32) for s in shapes),
        in_specs=[vm, vm],
        out_specs=(hbm, hbm),
        scratch_shapes=[pltpu.VMEM(s, F32) for s in shapes] + [pltpu.SemaphoreType.DMA((2,))],
        compiler_params=pltpu.CompilerParams(vmem_limit_bytes=12 * 1024 * 1024),
        cost_estimate=pl.CostEstimate(flops=1_000_000, bytes_accessed=4_000_000, transcendentals=0),
        name="node_out",
    )(mine, other)


def all_pieces(value, groups):
    return lax.all_to_all(value, ALL, 0, 0, axis_index_groups=groups, tiled=True)


def step(
    nodes,
    edges,
    node_cotangent,
    edge_cotangent,
    senders,
    receivers,
    send_lists,
    edge_first,
    edge_bias,
    edge_second,
    edge_gain,
    node_first,
    node_bias,
    node_second,
    node_gain,
):
    swap = [(0, 1), (1, 0)]
    count = lax.axis_size("space")
    onward = [(i, (i + 1) % count) for i in range(count)]
    backward = [((i + 1) % count, i) for i in range(count)]
    rows = nodes[0]
    lists = send_lists[0]
    D = rows.shape[1]
    H = edge_first.shape[1]
    halo = lists.shape[1]

    bias_row = edge_bias[None]
    first_other = lax.ppermute(edge_first, "hidden", swap)
    second_other = lax.ppermute(edge_second, "hidden", swap)
    bias_other = lax.ppermute(bias_row, "hidden", swap)
    list0, list1 = pick(lists, rows)
    from_prev = lax.ppermute(list1, "space", onward)
    from_next = lax.ppermute(list0, "space", backward)

    grads, dh, u, ndx = run_layer(
        (
            senders[None],
            receivers[None],
            rows,
            edge_first,
            bias_row,
            edges[0],
            edge_second,
            edge_gain[None],
            node_first,
            node_bias[None],
            node_second,
            node_gain[None],
            node_cotangent[0],
            edge_cotangent[0],
        ),
        (from_prev, from_next, first_other, bias_other, second_other),
    )
    pieces = all_pieces(grads, PLANES)
    gedges, gnodes, back_prev, back_next = run_inputs(
        edge_first, edge_cotangent[0], node_cotangent[0], first_other, dh, u, ndx, halo
    )
    from_next = lax.ppermute(back_prev, "space", backward)
    from_prev = lax.ppermute(back_next, "space", onward)
    pieces, from_next, from_prev = lax.optimization_barrier((pieces, from_next, from_prev))
    part = jnp.sum(pieces.astype(F32), axis=0).astype(BF)
    for bit in (2, 4):
        near = lax.ppermute(part, ALL, across_z(bit))
        part = (part.astype(F32) + near.astype(F32)).astype(BF)
    full = all_pieces(jnp.broadcast_to(part[None], (GROUP, *part.shape)), PLANES)
    grad_nodes = run_node(lists, gnodes, from_prev, from_next)

    split = (3 * D + 2 * H) // PIECE
    mine = full[2 * split :]
    other = lax.ppermute(mine, "hidden", swap)
    edge_first_grad, edge_second_grad, v0, v1, v2, v3 = run_edge_out(full, D, H)
    node_first_grad, node_second_grad = run_node_out(mine, other, D)
    return (
        grad_nodes[None],
        gedges[None],
        edge_first_grad,
        v0[0],
        edge_second_grad,
        v1[0],
        node_first_grad,
        v2[0],
        node_second_grad,
        v3[0],
    )


def solution(mesh):
    placed = (
        P("batch", "space", None),
        P("batch", "space", None),
        P("batch", "space", None),
        P("batch", "space", None),
        P("space"),
        P("space"),
        P("space", None, None),
        P(None, "hidden"),
        P("hidden"),
        P("hidden", None),
        P(),
        P(),
        P(),
        P(),
        P(),
    )
    return jax.shard_map(
        step,
        mesh=mesh,
        in_specs=placed,
        out_specs=(
            P("batch", "space", "hidden"),
            P("batch", "space", "hidden"),
            P(None, "hidden"),
            P("hidden"),
            P("hidden", None),
            P(),
            P(),
            P(),
            P(),
            P(),
        ),
        check_vma=False,
    )
```

```python
import jax
import jax.numpy as jnp
from jax import lax
from jax.experimental import pallas as pl
from jax.experimental.pallas import tpu as pltpu
from jax.sharding import PartitionSpec as P


EPS = 1e-05
BF = jnp.bfloat16
F32 = jnp.float32
ALL = ("batch", "space", "hidden")

NX, NY, NZ = 4, 4, 8
GROUP = 32
PIECE = 224
EXTRA = 8


def device_at(x, y, z, core):
    return ((y % 2) * 64 + (x * 2 + y // 2) * 8 + z) * 2 + core


def place_of(device):
    core, rest = device % 2, device // 2
    b, space = rest // 64, rest % 64
    return space // 16, (space // 8) % 2 * 2 + b, space % 8, core


PLANES = [
    [device_at(x, y, 2 * c + k, core) for x in range(NX) for y in range(NY) for k in range(2)]
    for core in range(2)
    for c in range(NZ // 2)
]


def across_z(first):
    pairs = []
    for device in range(2 * NX * NY * NZ):
        x, y, z, core = place_of(device)
        up = (z // 2) % 2 == (0 if first else 1)
        pairs.append((device, device_at(x, y, (z + (2 if up else NZ - 2)) % NZ, core)))
    return pairs


def dot(a, b):
    return jnp.dot(a, b, preferred_element_type=F32)


def dot_tn(a, b):
    return lax.dot_general(a, b, (((0,), (0,)), ((), ())), preferred_element_type=F32)


def dot_nt(a, b):
    return lax.dot_general(a, b, (((1,), (1,)), ((), ())), preferred_element_type=F32)


def silu_parts(pre):
    s = 0.5 * jnp.tanh(0.5 * pre) + 0.5
    return pre * s, s * (1.0 + pre * (1.0 - s))


def row_mean(v):
    return jnp.sum(v, axis=1, keepdims=True) * (1.0 / v.shape[1])


def normalize(z):
    centre = z - row_mean(z)
    scale = lax.rsqrt(row_mean(centre * centre) + EPS)
    return centre * scale, scale


def norm_back(g, normed, scale):
    return scale * (g - row_mean(g) - normed * row_mean(g * normed))


def in_hbm(*arrays):
    return tuple(pltpu.with_memory_space_constraint(a, pltpu.HBM) for a in arrays)


def own_columns(width):
    return pl.multiple_of(lax.axis_index("hidden") * width, width)


def copies(pairs, sems, first):
    return [pltpu.make_async_copy(a, b, sems.at[first + i]) for i, (a, b) in enumerate(pairs)]


def pick_kernel(lists, nodes, first, second, lists_v, nodes_v, sems):
    moves = copies([(lists, lists_v), (nodes, nodes_v)], sems, 0)
    for m in moves:
        m.start()
    for m in moves:
        m.wait()
    N, K = nodes_v.shape[0], lists_v.shape[1]
    for i, out in enumerate((first, second)):
        hot = lax.broadcasted_iota(jnp.int32, (N, K), 0) == lists_v[i : i + 1, :]
        out[...] = dot_tn(hot.astype(F32).astype(BF), nodes_v[...]).astype(BF)


def pick(lists, nodes):
    hbm = pl.BlockSpec(memory_space=pltpu.HBM)
    vm = pl.BlockSpec(memory_space=pltpu.VMEM)
    out = jax.ShapeDtypeStruct((lists.shape[1], nodes.shape[1]), BF)
    return pl.pallas_call(
        pick_kernel,
        out_shape=(out, out),
        in_specs=[hbm, hbm],
        out_specs=(vm, vm),
        scratch_shapes=[
            pltpu.VMEM(lists.shape, jnp.int32),
            pltpu.VMEM(nodes.shape, BF),
            pltpu.SemaphoreType.DMA((2,)),
        ],
        compiler_params=pltpu.CompilerParams(vmem_limit_bytes=4 * 1024 * 1024),
        cost_estimate=pl.CostEstimate(flops=200_000_000, bytes_accessed=400_000, transcendentals=0),
        name="pick",
    )(*in_hbm(lists, nodes))


LOADED = 14


def early_kernel(*refs):
    sources = refs[:LOADED]
    loaded = refs[LOADED : 2 * LOADED - 2]
    hot, part, snd, rcv, sems = refs[2 * LOADED - 2 :]
    moves = copies(list(zip(sources, (snd, rcv) + tuple(loaded))), sems, 0)
    for m in moves:
        m.start()
    nodes, w1m = loaded[0], loaded[1]
    D = nodes.shape[1]
    N, E = nodes.shape[0], snd.shape[1]
    T = hot.shape[0] - N
    for m in moves[0:2]:
        m.wait()
    hot[0:T, :] = (lax.broadcasted_iota(jnp.int32, (T, E), 0) == snd[...]).astype(F32).astype(BF)
    hot[T:, :] = (lax.broadcasted_iota(jnp.int32, (N, E), 0) == rcv[...]).astype(F32).astype(BF)
    for m in moves[2:4]:
        m.wait()
    part[0:N, :] = dot(nodes[...], w1m[D : 2 * D, :]).astype(BF)
    part[N:, :] = dot(nodes[...], w1m[2 * D :, :]).astype(BF)
    for m in moves[4:]:
        m.wait()


def run_early(params, halo):
    N = params[2].shape[0]
    E = params[5].shape[0]
    H = params[3].shape[1]
    hbm = pl.BlockSpec(memory_space=pltpu.HBM)
    vm = pl.BlockSpec(memory_space=pltpu.VMEM)
    outs = [pltpu.VMEM(p.shape, p.dtype) for p in params[2:]]
    outs += [pltpu.VMEM((2 * N + 2 * halo, E), BF), pltpu.VMEM((2 * N, H), BF)]
    return pl.pallas_call(
        early_kernel,
        out_shape=tuple(outs),
        in_specs=[hbm] * LOADED,
        out_specs=(vm,) * len(outs),
        scratch_shapes=[
            pltpu.VMEM(params[0].shape, jnp.int32),
            pltpu.VMEM(params[1].shape, jnp.int32),
            pltpu.SemaphoreType.DMA((LOADED,)),
        ],
        compiler_params=pltpu.CompilerParams(vmem_limit_bytes=8 * 1024 * 1024),
        cost_estimate=pl.CostEstimate(
            flops=1_500_000_000, bytes_accessed=8_000_000, transcendentals=0
        ),
        name="early",
    )(*in_hbm(*params))


def layer_kernel(*refs):
    loaded = refs[:LOADED]
    halo_p, halo_n, w1o, b1o, w2o = refs[LOADED : LOADED + 5]
    grads, gedges, gnodes, to_prev, to_next = refs[LOADED + 5 : LOADED + 10]
    (
        table,
        tw,
        act,
        slope,
        normed,
        scale,
        dz,
        dh,
        msum,
        ndh,
        ndz,
        ndx,
        aggr,
        ginp,
        ge,
        sems,
    ) = refs[LOADED + 10 :]
    nodes, w1m, b1m, edges, w2m, egain, nf, nb, ns, ngain, ncot, ecot, hot, early = loaded
    E, D = edges.shape
    N = nodes.shape[0]
    H = w1m.shape[1]
    T = table.shape[0]
    half = D // 2
    own = own_columns(half)
    side_rows = GROUP * PIECE // 2
    split = (3 * D + 2 * H) // PIECE

    def put(at, value):
        value = value.astype(BF)
        n = value.shape[0]
        done = 0
        while done < n:
            q, off = divmod(at + done, PIECE)
            take = min(n - done, PIECE - off)
            for side in range(2):
                if q < split:
                    piece = q + split * side
                else:
                    piece = 2 * split + (q - split) + (side_rows // PIECE - split) * side
                grads[piece, off : off + take, :] = value[
                    done : done + take, side * 128 : side * 128 + 128
                ]
            done += take

    table[0:N, :] = nodes[...]
    table[N : N + halo_p.shape[0], :] = halo_p[...]
    table[N + halo_p.shape[0] :, :] = halo_n[...]
    tw[0:N, 0:H] = early[0:N, :]
    tw[T:, 0:H] = early[N:, :]
    tw[N:T, 0:H] = dot(table[N:, :], w1m[D : 2 * D, :]).astype(BF)
    tw[0:T, H:] = dot(table[...], w1o[D : 2 * D, :]).astype(BF)
    tw[T:, H:] = dot(nodes[...], w1o[2 * D :, :]).astype(BF)
    bias = jnp.concatenate([b1m[...], b1o[...]], axis=1)
    aggr[...] = jnp.zeros_like(aggr)

    e = edges[...]
    pre = jnp.concatenate([dot(e, w1m[0:D, :]), dot(e, w1o[0:D, :])], axis=1)
    pre = pre + dot_tn(hot[...], tw[...]) + bias
    a, sl = silu_parts(pre)
    a = a.astype(BF)
    act[...] = a
    slope[...] = sl
    z = dot(a[:, 0:H], w2m[...]) + dot(a[:, H:], w2o[...])
    nz, sc = normalize(z)
    normed[...] = nz
    scale[...] = sc
    message = (egain[...] * nz).astype(BF)
    aggr[...] += dot(hot[T:, :], message)

    agg = aggr[...].astype(BF)
    ginp[:, 0:D] = nodes[...]
    ginp[:, D:] = agg
    npre = dot(ginp[...], nf[...]) + nb[...]
    nact, nslope = silu_parts(npre)
    nact = nact.astype(BF)
    nnorm, nscale = normalize(dot(nact, ns[...]))
    up = ncot[...].astype(F32)
    gain_n = jnp.sum(up * nnorm, axis=0, keepdims=True)
    dzn = norm_back(ngain[...] * up, nnorm, nscale).astype(BF)
    ndz[...] = dzn
    dhn = (dot_nt(dzn, ns[...]) * nslope).astype(BF)
    ndh[...] = dhn
    bias_n = jnp.sum(dhn.astype(F32), axis=0, keepdims=True)
    put(3 * D + 2 * H, dot_tn(ginp[...], ndh[:, pl.ds(own, half)]))
    put(5 * D + 2 * H, dot_tn(nact, ndz[:, pl.ds(own, half)]))
    dxn = dot_nt(dhn, nf[...])
    ndx[...] = dxn[:, 0:D]
    ag = dxn[:, D:].astype(BF)
    msum[...] = jnp.zeros_like(msum)

    mg = ecot[...].astype(F32) + dot_tn(hot[T:, :], ag)
    nz = normed[...]
    msum[0:8, :] += jnp.sum((mg * nz).reshape(E // 8, 8, D), axis=0)
    d = norm_back(egain[...] * mg, nz, scale[...]).astype(BF)
    dz[...] = d
    g = jnp.concatenate([dot_nt(d, w2m[...]), dot_nt(d, w2o[...])], axis=1)
    g = (g * slope[...]).astype(BF)
    dh[...] = g
    msum[8:16, :] += jnp.sum(g.astype(F32).reshape(E // 8, 8, D), axis=0)
    part = dot_nt(g[:, 0:H], w1m[pl.ds(own, half), :]) + dot_nt(
        g[:, H:], w1o[pl.ds(own, half), :]
    )
    ge[...] = (ecot[:, pl.ds(own, half)].astype(F32) + part).astype(BF)

    last = pltpu.make_async_copy(ge, gedges, sems.at[0])
    last.start()
    u = dot(hot[...], dh[...]).astype(BF)
    K = halo_p.shape[0]
    at_s = pl.ds(pl.multiple_of(D + own, half), half)
    at_r = pl.ds(pl.multiple_of(2 * D + own, half), half)
    tg = dot_nt(u[0:T, 0:H], w1m[at_s, :]) + dot_nt(u[0:T, H:], w1o[at_s, :])
    rg = dot_nt(u[T:, 0:H], w1m[at_r, :]) + dot_nt(u[T:, H:], w1o[at_r, :])
    to_prev[...] = tg[N : N + K, :].astype(BF)
    to_next[...] = tg[N + K :, :].astype(BF)
    gnodes[...] = ncot[:, pl.ds(own, half)].astype(F32) + ndx[:, pl.ds(own, half)] + tg[0:N] + rg
    second = dot_tn(act[:, 0:H], dz[...])
    put(3 * D, second[:, 0:half])
    put(3 * D + H, second[:, half:])
    put(0, dot_tn(edges[...], dh[:, 0:H]))
    put(D, dot_tn(table[...], u[0:T, 0:H]))
    put(2 * D, dot_tn(nodes[...], u[T:, 0:H]))

    gain_e = jnp.sum(msum[0:8, :], axis=0, keepdims=True)
    bias_e = jnp.sum(msum[8:16, :], axis=0, keepdims=True)[:, 0:H]
    parts = []
    for v in (bias_e, gain_e, bias_n, gain_n):
        parts += [v[:, i : i + 128] for i in range(0, v.shape[1], 128)]
    zero = jnp.zeros((2 * EXTRA - len(parts), 128), F32)
    vec = jnp.concatenate(parts + [zero], axis=0).astype(BF)
    for piece in range(GROUP):
        if piece < 2:
            grads[piece, PIECE:, :] = vec[piece * EXTRA : piece * EXTRA + EXTRA]
        else:
            grads[piece, PIECE:, :] = jnp.zeros((EXTRA, 128), BF)
    last.wait()


LAYER_VMEM = 26 * 1024 * 1024


def run_layer(params, arrived):
    N, D = params[0].shape
    H = params[1].shape[1]
    E = params[3].shape[0]
    T = N + 2 * arrived[0].shape[0]
    hbm = pl.BlockSpec(memory_space=pltpu.HBM)
    vm = pl.BlockSpec(memory_space=pltpu.VMEM)
    return pl.pallas_call(
        layer_kernel,
        out_shape=(
            jax.ShapeDtypeStruct((GROUP, PIECE + EXTRA, 128), BF),
            jax.ShapeDtypeStruct((E, D // 2), BF),
            jax.ShapeDtypeStruct((N, D // 2), F32),
            jax.ShapeDtypeStruct((arrived[0].shape[0], D // 2), BF),
            jax.ShapeDtypeStruct((arrived[0].shape[0], D // 2), BF),
        ),
        in_specs=[vm] * (LOADED + len(arrived)),
        out_specs=(vm, hbm, vm, vm, vm),
        scratch_shapes=[
            pltpu.VMEM((T, D), BF),
            pltpu.VMEM((T + N, 2 * H), BF),
            pltpu.VMEM((E, 2 * H), BF),
            pltpu.VMEM((E, 2 * H), F32),
            pltpu.VMEM((E, D), F32),
            pltpu.VMEM((E, 1), F32),
            pltpu.VMEM((E, D), BF),
            pltpu.VMEM((E, 2 * H), BF),
            pltpu.VMEM((16, D), F32),
            pltpu.VMEM((N, D), BF),
            pltpu.VMEM((N, D), BF),
            pltpu.VMEM((N, D), F32),
            pltpu.VMEM((N, D), F32),
            pltpu.VMEM((N, 2 * D), BF),
            pltpu.VMEM((E, D // 2), BF),
            pltpu.SemaphoreType.DMA((1,)),
        ],
        compiler_params=pltpu.CompilerParams(vmem_limit_bytes=LAYER_VMEM),
        cost_estimate=pl.CostEstimate(
            flops=6_000_000_000, bytes_accessed=12_000_000, transcendentals=1_000_000
        ),
        name="layer",
    )(*params, *arrived)


def node_kernel(lists, gnodes, first, second, out, lists_v, sems):
    move = pltpu.make_async_copy(lists, lists_v, sems.at[0])
    move.start()
    move.wait()
    N, K = gnodes.shape[0], first.shape[0]
    total = gnodes[...]
    for i, value in enumerate((first, second)):
        hot = lax.broadcasted_iota(jnp.int32, (N, K), 0) == lists_v[i : i + 1, :]
        total = total + dot(hot.astype(F32).astype(BF), value[...])
    out[...] = total.astype(BF)


def run_node(lists, gnodes, first, second):
    hbm = pl.BlockSpec(memory_space=pltpu.HBM)
    vm = pl.BlockSpec(memory_space=pltpu.VMEM)
    return pl.pallas_call(
        node_kernel,
        out_shape=jax.ShapeDtypeStruct(gnodes.shape, BF),
        in_specs=[hbm, vm, vm, vm],
        out_specs=vm,
        scratch_shapes=[pltpu.VMEM(lists.shape, jnp.int32), pltpu.SemaphoreType.DMA((1,))],
        compiler_params=pltpu.CompilerParams(vmem_limit_bytes=4 * 1024 * 1024),
        cost_estimate=pl.CostEstimate(flops=100_000_000, bytes_accessed=300_000, transcendentals=0),
        name="node_gradient",
    )(*in_hbm(lists), gnodes, first, second)


def edge_out_kernel(
    full, first, second, v0, v1, v2, v3, nfirst, nsecond, first_v, second_v, nfirst_v, nsecond_v, sems
):
    D3, _ = first.shape
    H = second.shape[0]
    half = second.shape[1] // 2
    split = (D3 + 2 * H) // PIECE
    last = GROUP // 2 - split

    def fetch(at, count, put):
        done = 0
        while done < count:
            q, off = divmod(at + done, PIECE)
            take = min(count - done, PIECE - off)
            for side in range(2):
                if q < split:
                    piece = q + split * side
                else:
                    piece = 2 * split + (q - split) + last * side
                put(done, take, side, full[piece, off : off + take, :].astype(F32))
            done += take

    def put_first(done, take, side, value):
        first_v[done : done + take, side * 128 : side * 128 + 128] = value

    fetch(0, D3, put_first)
    D2, D = nfirst.shape
    cols = pl.ds(own_columns(D // 2), D // 2)
    moves = copies(
        [
            (first_v, first),
            (second_v, second),
            (nfirst_v, nfirst.at[:, cols]),
            (nsecond_v, nsecond.at[:, cols]),
        ],
        sems,
        0,
    )
    moves[0].start()
    for part in range(2):

        def put_second(done, take, side, value):
            at = part * half + side * 128
            second_v[done : done + take, at : at + 128] = value

        fetch(D3 + part * H, H, put_second)
    moves[1].start()
    for base, count, target, move in (
        (D3 + 2 * H, D2, nfirst_v, moves[2]),
        (D3 + 2 * H + D2, D, nsecond_v, moves[3]),
    ):

        def put_node(done, take, side, value):
            target[done : done + take, side * 128 : side * 128 + 128] = value

        fetch(base, count, put_node)
        move.start()
    row = 0
    for out in (v0, v1, v2, v3):
        for at in range(0, out.shape[1], 128):
            piece, off = divmod(row, EXTRA)
            tile = full[piece, PIECE:, :].astype(F32)
            out[:, at : at + 128] = tile[off : off + 1, :]
            row += 1
    for m in moves:
        m.wait()


def run_edge_out(full, D, H):
    hbm = pl.BlockSpec(memory_space=pltpu.HBM)
    vm = pl.BlockSpec(memory_space=pltpu.VMEM)
    shapes = [(3 * D, H), (H, D)]
    outs = shapes + [(1, H), (1, D), (1, D), (1, D), (2 * D, D), (D, D)]
    held = shapes + [(2 * D, D // 2), (D, D // 2)]
    return pl.pallas_call(
        edge_out_kernel,
        out_shape=tuple(jax.ShapeDtypeStruct(s, F32) for s in outs),
        in_specs=[vm],
        out_specs=(hbm, hbm, vm, vm, vm, vm, hbm, hbm),
        scratch_shapes=[pltpu.VMEM(s, F32) for s in held] + [pltpu.SemaphoreType.DMA((4,))],
        compiler_params=pltpu.CompilerParams(vmem_limit_bytes=12 * 1024 * 1024),
        cost_estimate=pl.CostEstimate(flops=1_000_000, bytes_accessed=5_000_000, transcendentals=0),
        name="edge_out",
    )(full)


def node_out_kernel(other, first_in, second_in, first, second, first_v, second_v, sems):
    D2, D = first.shape
    half = D // 2
    cols = pl.ds(pl.multiple_of(half - own_columns(half), half), half)
    skip = (3 * D + D2 // 2) % PIECE
    last = other.shape[0] // 2
    moves = copies([(first_v, first.at[:, cols]), (second_v, second.at[:, cols])], sems, 0)
    for base, count, out, move in ((0, D2, first_v, moves[0]), (D2, D, second_v, moves[1])):
        done = 0
        while done < count:
            q, off = divmod(skip + base + done, PIECE)
            take = min(count - done, PIECE - off)
            for side in range(2):
                out[done : done + take, side * 128 : side * 128 + 128] = other[
                    q + last * side, off : off + take, :
                ].astype(F32)
            done += take
        move.start()
    for m in moves:
        m.wait()


def run_node_out(other, first, second):
    hbm = pl.BlockSpec(memory_space=pltpu.HBM)
    vm = pl.BlockSpec(memory_space=pltpu.VMEM)
    shapes = [first.shape, second.shape]
    return pl.pallas_call(
        node_out_kernel,
        out_shape=tuple(jax.ShapeDtypeStruct(s, F32) for s in shapes),
        in_specs=[vm, hbm, hbm],
        out_specs=(hbm, hbm),
        input_output_aliases={1: 0, 2: 1},
        scratch_shapes=[pltpu.VMEM((s[0], s[1] // 2), F32) for s in shapes]
        + [pltpu.SemaphoreType.DMA((2,))],
        compiler_params=pltpu.CompilerParams(vmem_limit_bytes=12 * 1024 * 1024),
        cost_estimate=pl.CostEstimate(flops=1_000_000, bytes_accessed=2_000_000, transcendentals=0),
        name="node_out",
    )(other, first, second)


def sum_kernel(pieces, out):
    def add(at):
        total = pieces[0, at, :].astype(F32)
        for p in range(1, pieces.shape[0]):
            total = total + pieces[p, at, :].astype(F32)
        out[at, :] = total.astype(BF)

    step = 32

    @pl.loop(0, PIECE // step)
    def _(i):
        add(pl.ds(pl.multiple_of(i * step, step), step))

    add(slice(PIECE, PIECE + EXTRA))


def run_sum(pieces):
    vm = pl.BlockSpec(memory_space=pltpu.VMEM)
    return pl.pallas_call(
        sum_kernel,
        out_shape=jax.ShapeDtypeStruct(pieces.shape[1:], BF),
        in_specs=[vm],
        out_specs=vm,
        compiler_params=pltpu.CompilerParams(vmem_limit_bytes=4 * 1024 * 1024),
        cost_estimate=pl.CostEstimate(flops=1_000_000, bytes_accessed=2_000_000, transcendentals=0),
        name="sum_pieces",
    )(pieces)


def all_pieces(value, groups):
    return lax.all_to_all(value, ALL, 0, 0, axis_index_groups=groups, tiled=True)


def step(
    nodes,
    edges,
    node_cotangent,
    edge_cotangent,
    senders,
    receivers,
    send_lists,
    edge_first,
    edge_bias,
    edge_second,
    edge_gain,
    node_first,
    node_bias,
    node_second,
    node_gain,
):
    swap = [(0, 1), (1, 0)]
    count = lax.axis_size("space")
    onward = [(i, (i + 1) % count) for i in range(count)]
    backward = [((i + 1) % count, i) for i in range(count)]
    rows = nodes[0]
    lists = send_lists[0]
    D = rows.shape[1]
    H = edge_first.shape[1]
    halo = lists.shape[1]

    bias_row = edge_bias[None]
    first_other = lax.ppermute(edge_first, "hidden", swap)
    second_other = lax.ppermute(edge_second, "hidden", swap)
    bias_other = lax.ppermute(bias_row, "hidden", swap)
    list0, list1 = pick(lists, rows)
    from_prev = lax.ppermute(list1, "space", onward)
    from_next = lax.ppermute(list0, "space", backward)

    ready = run_early(
        (
            senders[None],
            receivers[None],
            rows,
            edge_first,
            bias_row,
            edges[0],
            edge_second,
            edge_gain[None],
            node_first,
            node_bias[None],
            node_second,
            node_gain[None],
            node_cotangent[0],
            edge_cotangent[0],
        ),
        halo,
    )
    grads, gedges, gnodes, back_prev, back_next = run_layer(
        ready,
        (from_prev, from_next, first_other, bias_other, second_other),
    )
    from_next = lax.ppermute(back_prev, "space", backward)
    from_prev = lax.ppermute(back_next, "space", onward)
    pieces = all_pieces(grads, PLANES)
    part = run_sum(pieces)
    other = lax.ppermute(part, ALL, across_z(True))
    part = (part.astype(F32) + other.astype(F32)).astype(BF)
    other = lax.ppermute(part, ALL, across_z(False))
    grad_nodes = run_node(lists, gnodes, from_prev, from_next)
    part = (part.astype(F32) + other.astype(F32)).astype(BF)
    copied = jnp.broadcast_to(part[None], (GROUP, *part.shape))
    full = all_pieces(copied, PLANES)

    split = (3 * D + 2 * H) // PIECE
    mine = full[2 * split :]
    other = lax.ppermute(mine, "hidden", swap)
    edge_first_grad, edge_second_grad, v0, v1, v2, v3, nfirst, nsecond = run_edge_out(full, D, H)
    node_first_grad, node_second_grad = run_node_out(other, nfirst, nsecond)
    return (
        grad_nodes[None],
        gedges[None],
        edge_first_grad,
        v0[0],
        edge_second_grad,
        v1[0],
        node_first_grad,
        v2[0],
        node_second_grad,
        v3[0],
    )


def solution(mesh):
    placed = (
        P("batch", "space", None),
        P("batch", "space", None),
        P("batch", "space", None),
        P("batch", "space", None),
        P("space"),
        P("space"),
        P("space", None, None),
        P(None, "hidden"),
        P("hidden"),
        P("hidden", None),
        P(),
        P(),
        P(),
        P(),
        P(),
    )
    return jax.shard_map(
        step,
        mesh=mesh,
        in_specs=placed,
        out_specs=(
            P("batch", "space", "hidden"),
            P("batch", "space", "hidden"),
            P(None, "hidden"),
            P("hidden"),
            P("hidden", None),
            P(),
            P(),
            P(),
            P(),
            P(),
        ),
        check_vma=False,
    )
```

```python
import jax
import jax.numpy as jnp
from jax import lax
from jax.experimental import pallas as pl
from jax.experimental.pallas import tpu as pltpu
from jax.sharding import PartitionSpec as P


EPS = 1e-05
BF = jnp.bfloat16
F32 = jnp.float32
ALL = ("batch", "space", "hidden")

NX, NY, NZ = 4, 4, 8
GROUP = 32
PIECE = 224
EXTRA = 8


def device_at(x, y, z, core):
    return ((y % 2) * 64 + (x * 2 + y // 2) * 8 + z) * 2 + core


def place_of(device):
    core, rest = device % 2, device // 2
    b, space = rest // 64, rest % 64
    return space // 16, (space // 8) % 2 * 2 + b, space % 8, core


PLANES = [
    [device_at(x, y, 2 * c + k, core) for x in range(NX) for y in range(NY) for k in range(2)]
    for core in range(2)
    for c in range(NZ // 2)
]


def across_z(first):
    pairs = []
    for device in range(2 * NX * NY * NZ):
        x, y, z, core = place_of(device)
        up = (z // 2) % 2 == (0 if first else 1)
        pairs.append((device, device_at(x, y, (z + (2 if up else NZ - 2)) % NZ, core)))
    return pairs


def dot(a, b):
    return jnp.dot(a, b, preferred_element_type=F32)


def dot_tn(a, b):
    return lax.dot_general(a, b, (((0,), (0,)), ((), ())), preferred_element_type=F32)


def dot_nt(a, b):
    return lax.dot_general(a, b, (((1,), (1,)), ((), ())), preferred_element_type=F32)


def silu_parts(pre):
    s = 0.5 * jnp.tanh(0.5 * pre) + 0.5
    return pre * s, s * (1.0 + pre * (1.0 - s))


def row_mean(v):
    return jnp.sum(v, axis=1, keepdims=True) * (1.0 / v.shape[1])


def normalize(z):
    centre = z - row_mean(z)
    scale = lax.rsqrt(row_mean(centre * centre) + EPS)
    return centre * scale, scale


def norm_back(g, normed, scale):
    return scale * (g - row_mean(g) - normed * row_mean(g * normed))


def in_hbm(*arrays):
    return tuple(pltpu.with_memory_space_constraint(a, pltpu.HBM) for a in arrays)


def own_columns(width):
    return pl.multiple_of(lax.axis_index("hidden") * width, width)


def copies(pairs, sems, first):
    return [pltpu.make_async_copy(a, b, sems.at[first + i]) for i, (a, b) in enumerate(pairs)]


def pick_kernel(lists, nodes, first, second, lists_v, nodes_v, sems):
    moves = copies([(lists, lists_v), (nodes, nodes_v)], sems, 0)
    for m in moves:
        m.start()
    for m in moves:
        m.wait()
    N, K = nodes_v.shape[0], lists_v.shape[1]
    for i, out in enumerate((first, second)):
        hot = lax.broadcasted_iota(jnp.int32, (N, K), 0) == lists_v[i : i + 1, :]
        out[...] = dot_tn(hot.astype(F32).astype(BF), nodes_v[...]).astype(BF)


def pick(lists, nodes):
    hbm = pl.BlockSpec(memory_space=pltpu.HBM)
    vm = pl.BlockSpec(memory_space=pltpu.VMEM)
    out = jax.ShapeDtypeStruct((lists.shape[1], nodes.shape[1]), BF)
    return pl.pallas_call(
        pick_kernel,
        out_shape=(out, out),
        in_specs=[hbm, hbm],
        out_specs=(vm, vm),
        scratch_shapes=[
            pltpu.VMEM(lists.shape, jnp.int32),
            pltpu.VMEM(nodes.shape, BF),
            pltpu.SemaphoreType.DMA((2,)),
        ],
        compiler_params=pltpu.CompilerParams(vmem_limit_bytes=4 * 1024 * 1024),
        cost_estimate=pl.CostEstimate(flops=200_000_000, bytes_accessed=400_000, transcendentals=0),
        name="pick",
    )(*in_hbm(lists, nodes))


LOADED = 14


def early_kernel(*refs):
    sources = refs[:LOADED]
    loaded = refs[LOADED : 2 * LOADED - 2]
    hot, part, snd, rcv, sems = refs[2 * LOADED - 2 :]
    moves = copies(list(zip(sources, (snd, rcv) + tuple(loaded))), sems, 0)
    for m in moves:
        m.start()
    nodes, w1m = loaded[0], loaded[1]
    D = nodes.shape[1]
    N, E = nodes.shape[0], snd.shape[1]
    T = hot.shape[0] - N
    for m in moves[0:2]:
        m.wait()
    hot[0:T, :] = (lax.broadcasted_iota(jnp.int32, (T, E), 0) == snd[...]).astype(F32).astype(BF)
    hot[T:, :] = (lax.broadcasted_iota(jnp.int32, (N, E), 0) == rcv[...]).astype(F32).astype(BF)
    for m in moves[2:4]:
        m.wait()
    part[0:N, :] = dot(nodes[...], w1m[D : 2 * D, :]).astype(BF)
    part[N:, :] = dot(nodes[...], w1m[2 * D :, :]).astype(BF)
    for m in moves[4:]:
        m.wait()


def run_early(params, halo):
    N = params[2].shape[0]
    E = params[5].shape[0]
    H = params[3].shape[1]
    hbm = pl.BlockSpec(memory_space=pltpu.HBM)
    vm = pl.BlockSpec(memory_space=pltpu.VMEM)
    outs = [pltpu.VMEM(p.shape, p.dtype) for p in params[2:]]
    outs += [pltpu.VMEM((2 * N + 2 * halo, E), BF), pltpu.VMEM((2 * N, H), BF)]
    return pl.pallas_call(
        early_kernel,
        out_shape=tuple(outs),
        in_specs=[hbm] * LOADED,
        out_specs=(vm,) * len(outs),
        scratch_shapes=[
            pltpu.VMEM(params[0].shape, jnp.int32),
            pltpu.VMEM(params[1].shape, jnp.int32),
            pltpu.SemaphoreType.DMA((LOADED,)),
        ],
        compiler_params=pltpu.CompilerParams(vmem_limit_bytes=8 * 1024 * 1024),
        cost_estimate=pl.CostEstimate(
            flops=1_500_000_000, bytes_accessed=8_000_000, transcendentals=0
        ),
        name="early",
    )(*in_hbm(*params))


def layer_kernel(*refs):
    loaded = refs[:LOADED]
    halo_p, halo_n, w1o, b1o, w2o = refs[LOADED : LOADED + 5]
    grads, gedges, gnodes, to_prev, to_next = refs[LOADED + 5 : LOADED + 10]
    (
        table,
        tw,
        act,
        slope,
        normed,
        scale,
        dz,
        dh,
        msum,
        ndh,
        ndz,
        ndx,
        aggr,
        ginp,
        ge,
        sems,
    ) = refs[LOADED + 10 :]
    nodes, w1m, b1m, edges, w2m, egain, nf, nb, ns, ngain, ncot, ecot, hot, early = loaded
    E, D = edges.shape
    N = nodes.shape[0]
    H = w1m.shape[1]
    T = table.shape[0]
    half = D // 2
    own = own_columns(half)
    side_rows = GROUP * PIECE // 2
    split = (3 * D + 2 * H) // PIECE

    def put(at, value):
        value = value.astype(BF)
        n = value.shape[0]
        done = 0
        while done < n:
            q, off = divmod(at + done, PIECE)
            take = min(n - done, PIECE - off)
            for side in range(2):
                if q < split:
                    piece = q + split * side
                else:
                    piece = 2 * split + (q - split) + (side_rows // PIECE - split) * side
                grads[piece, off : off + take, :] = value[
                    done : done + take, side * 128 : side * 128 + 128
                ]
            done += take

    table[0:N, :] = nodes[...]
    table[N : N + halo_p.shape[0], :] = halo_p[...]
    table[N + halo_p.shape[0] :, :] = halo_n[...]
    tw[0:N, 0:H] = early[0:N, :]
    tw[T:, 0:H] = early[N:, :]
    tw[N:T, 0:H] = dot(table[N:, :], w1m[D : 2 * D, :]).astype(BF)
    tw[0:T, H:] = dot(table[...], w1o[D : 2 * D, :]).astype(BF)
    tw[T:, H:] = dot(nodes[...], w1o[2 * D :, :]).astype(BF)
    bias = jnp.concatenate([b1m[...], b1o[...]], axis=1)
    aggr[...] = jnp.zeros_like(aggr)

    e = edges[...]
    pre = jnp.concatenate([dot(e, w1m[0:D, :]), dot(e, w1o[0:D, :])], axis=1)
    pre = pre + dot_tn(hot[...], tw[...]) + bias
    a, sl = silu_parts(pre)
    a = a.astype(BF)
    act[...] = a
    slope[...] = sl
    z = dot(a[:, 0:H], w2m[...]) + dot(a[:, H:], w2o[...])
    nz, sc = normalize(z)
    normed[...] = nz
    scale[...] = sc
    message = (egain[...] * nz).astype(BF)
    aggr[...] += dot(hot[T:, :], message)

    agg = aggr[...].astype(BF)
    ginp[:, 0:D] = nodes[...]
    ginp[:, D:] = agg
    npre = dot(ginp[...], nf[...]) + nb[...]
    nact, nslope = silu_parts(npre)
    nact = nact.astype(BF)
    nnorm, nscale = normalize(dot(nact, ns[...]))
    up = ncot[...].astype(F32)
    gain_n = jnp.sum(up * nnorm, axis=0, keepdims=True)
    dzn = norm_back(ngain[...] * up, nnorm, nscale).astype(BF)
    ndz[...] = dzn
    dhn = (dot_nt(dzn, ns[...]) * nslope).astype(BF)
    ndh[...] = dhn
    bias_n = jnp.sum(dhn.astype(F32), axis=0, keepdims=True)
    put(3 * D + 2 * H, dot_tn(ginp[...], ndh[:, pl.ds(own, half)]))
    put(5 * D + 2 * H, dot_tn(nact, ndz[:, pl.ds(own, half)]))
    dxn = dot_nt(dhn, nf[...])
    ndx[...] = dxn[:, 0:D]
    ag = dxn[:, D:].astype(BF)
    msum[...] = jnp.zeros_like(msum)

    mg = ecot[...].astype(F32) + dot_tn(hot[T:, :], ag)
    nz = normed[...]
    msum[0:8, :] += jnp.sum((mg * nz).reshape(E // 8, 8, D), axis=0)
    d = norm_back(egain[...] * mg, nz, scale[...]).astype(BF)
    dz[...] = d
    g = jnp.concatenate([dot_nt(d, w2m[...]), dot_nt(d, w2o[...])], axis=1)
    g = (g * slope[...]).astype(BF)
    dh[...] = g
    msum[8:16, :] += jnp.sum(g.astype(F32).reshape(E // 8, 8, D), axis=0)
    part = dot_nt(g[:, 0:H], w1m[pl.ds(own, half), :]) + dot_nt(
        g[:, H:], w1o[pl.ds(own, half), :]
    )
    ge[...] = (ecot[:, pl.ds(own, half)].astype(F32) + part).astype(BF)

    last = pltpu.make_async_copy(ge, gedges, sems.at[0])
    last.start()
    u = dot(hot[...], dh[...]).astype(BF)
    K = halo_p.shape[0]
    at_s = pl.ds(pl.multiple_of(D + own, half), half)
    at_r = pl.ds(pl.multiple_of(2 * D + own, half), half)
    tg = dot_nt(u[0:T, 0:H], w1m[at_s, :]) + dot_nt(u[0:T, H:], w1o[at_s, :])
    rg = dot_nt(u[T:, 0:H], w1m[at_r, :]) + dot_nt(u[T:, H:], w1o[at_r, :])
    to_prev[...] = tg[N : N + K, :].astype(BF)
    to_next[...] = tg[N + K :, :].astype(BF)
    gnodes[...] = ncot[:, pl.ds(own, half)].astype(F32) + ndx[:, pl.ds(own, half)] + tg[0:N] + rg
    second = dot_tn(act[:, 0:H], dz[...])
    put(3 * D, second[:, 0:half])
    put(3 * D + H, second[:, half:])
    put(0, dot_tn(edges[...], dh[:, 0:H]))
    put(D, dot_tn(table[...], u[0:T, 0:H]))
    put(2 * D, dot_tn(nodes[...], u[T:, 0:H]))

    gain_e = jnp.sum(msum[0:8, :], axis=0, keepdims=True)
    bias_e = jnp.sum(msum[8:16, :], axis=0, keepdims=True)[:, 0:H]
    parts = []
    for v in (bias_e, gain_e, bias_n, gain_n):
        parts += [v[:, i : i + 128] for i in range(0, v.shape[1], 128)]
    zero = jnp.zeros((2 * EXTRA - len(parts), 128), F32)
    vec = jnp.concatenate(parts + [zero], axis=0).astype(BF)
    for piece in range(GROUP):
        if piece < 2:
            grads[piece, PIECE:, :] = vec[piece * EXTRA : piece * EXTRA + EXTRA]
        else:
            grads[piece, PIECE:, :] = jnp.zeros((EXTRA, 128), BF)
    last.wait()


LAYER_VMEM = 26 * 1024 * 1024


def run_layer(params, arrived):
    N, D = params[0].shape
    H = params[1].shape[1]
    E = params[3].shape[0]
    T = N + 2 * arrived[0].shape[0]
    hbm = pl.BlockSpec(memory_space=pltpu.HBM)
    vm = pl.BlockSpec(memory_space=pltpu.VMEM)
    return pl.pallas_call(
        layer_kernel,
        out_shape=(
            jax.ShapeDtypeStruct((GROUP, PIECE + EXTRA, 128), BF),
            jax.ShapeDtypeStruct((E, D // 2), BF),
            jax.ShapeDtypeStruct((N, D // 2), F32),
            jax.ShapeDtypeStruct((arrived[0].shape[0], D // 2), BF),
            jax.ShapeDtypeStruct((arrived[0].shape[0], D // 2), BF),
        ),
        in_specs=[vm] * (LOADED + len(arrived)),
        out_specs=(vm, hbm, vm, vm, vm),
        scratch_shapes=[
            pltpu.VMEM((T, D), BF),
            pltpu.VMEM((T + N, 2 * H), BF),
            pltpu.VMEM((E, 2 * H), BF),
            pltpu.VMEM((E, 2 * H), F32),
            pltpu.VMEM((E, D), F32),
            pltpu.VMEM((E, 1), F32),
            pltpu.VMEM((E, D), BF),
            pltpu.VMEM((E, 2 * H), BF),
            pltpu.VMEM((16, D), F32),
            pltpu.VMEM((N, D), BF),
            pltpu.VMEM((N, D), BF),
            pltpu.VMEM((N, D), F32),
            pltpu.VMEM((N, D), F32),
            pltpu.VMEM((N, 2 * D), BF),
            pltpu.VMEM((E, D // 2), BF),
            pltpu.SemaphoreType.DMA((1,)),
        ],
        compiler_params=pltpu.CompilerParams(vmem_limit_bytes=LAYER_VMEM),
        cost_estimate=pl.CostEstimate(
            flops=6_000_000_000, bytes_accessed=12_000_000, transcendentals=1_000_000
        ),
        name="layer",
    )(*params, *arrived)


def edge_out_kernel(
    full,
    lists,
    gnodes,
    back_p,
    back_n,
    first,
    second,
    v0,
    v1,
    v2,
    v3,
    nfirst,
    nsecond,
    gout,
    first_v,
    second_v,
    nfirst_v,
    nsecond_v,
    lists_v,
    sems,
):
    asked = pltpu.make_async_copy(lists, lists_v, sems.at[4])
    asked.start()
    D3, _ = first.shape
    H = second.shape[0]
    half = second.shape[1] // 2
    split = (D3 + 2 * H) // PIECE
    last = GROUP // 2 - split

    def fetch(at, count, put):
        done = 0
        while done < count:
            q, off = divmod(at + done, PIECE)
            take = min(count - done, PIECE - off)
            for side in range(2):
                if q < split:
                    piece = q + split * side
                else:
                    piece = 2 * split + (q - split) + last * side
                put(done, take, side, full[piece, off : off + take, :].astype(F32))
            done += take

    def put_first(done, take, side, value):
        first_v[done : done + take, side * 128 : side * 128 + 128] = value

    fetch(0, D3, put_first)
    D2, D = nfirst.shape
    cols = pl.ds(own_columns(D // 2), D // 2)
    moves = copies(
        [
            (first_v, first),
            (second_v, second),
            (nfirst_v, nfirst.at[:, cols]),
            (nsecond_v, nsecond.at[:, cols]),
        ],
        sems,
        0,
    )
    moves[0].start()
    for part in range(2):

        def put_second(done, take, side, value):
            at = part * half + side * 128
            second_v[done : done + take, at : at + 128] = value

        fetch(D3 + part * H, H, put_second)
    moves[1].start()
    for base, count, target, move in (
        (D3 + 2 * H, D2, nfirst_v, moves[2]),
        (D3 + 2 * H + D2, D, nsecond_v, moves[3]),
    ):

        def put_node(done, take, side, value):
            target[done : done + take, side * 128 : side * 128 + 128] = value

        fetch(base, count, put_node)
        move.start()
    row = 0
    for out in (v0, v1, v2, v3):
        for at in range(0, out.shape[1], 128):
            piece, off = divmod(row, EXTRA)
            tile = full[piece, PIECE:, :].astype(F32)
            out[:, at : at + 128] = tile[off : off + 1, :]
            row += 1
    asked.wait()
    N, K = gnodes.shape[0], back_p.shape[0]
    total = gnodes[...]
    for i, value in enumerate((back_p, back_n)):
        hot = lax.broadcasted_iota(jnp.int32, (N, K), 0) == lists_v[i : i + 1, :]
        total = total + dot(hot.astype(F32).astype(BF), value[...])
    gout[...] = total.astype(BF)
    for m in moves:
        m.wait()


def run_edge_out(full, lists, gnodes, back_p, back_n, D, H):
    hbm = pl.BlockSpec(memory_space=pltpu.HBM)
    vm = pl.BlockSpec(memory_space=pltpu.VMEM)
    shapes = [(3 * D, H), (H, D)]
    outs = shapes + [(1, H), (1, D), (1, D), (1, D), (2 * D, D), (D, D)]
    held = shapes + [(2 * D, D // 2), (D, D // 2)]
    return pl.pallas_call(
        edge_out_kernel,
        out_shape=tuple(jax.ShapeDtypeStruct(s, F32) for s in outs)
        + (jax.ShapeDtypeStruct(gnodes.shape, BF),),
        in_specs=[vm, hbm, vm, vm, vm],
        out_specs=(hbm, hbm, vm, vm, vm, vm, hbm, hbm, vm),
        scratch_shapes=[pltpu.VMEM(s, F32) for s in held]
        + [pltpu.VMEM(lists.shape, jnp.int32), pltpu.SemaphoreType.DMA((5,))],
        compiler_params=pltpu.CompilerParams(vmem_limit_bytes=12 * 1024 * 1024),
        cost_estimate=pl.CostEstimate(flops=1_000_000, bytes_accessed=5_000_000, transcendentals=0),
        name="edge_out",
    )(full, *in_hbm(lists), gnodes, back_p, back_n)


def node_out_kernel(other, first_in, second_in, first, second, first_v, second_v, sems):
    D2, D = first.shape
    half = D // 2
    cols = pl.ds(pl.multiple_of(half - own_columns(half), half), half)
    skip = (3 * D + D2 // 2) % PIECE
    last = other.shape[0] // 2
    moves = copies([(first_v, first.at[:, cols]), (second_v, second.at[:, cols])], sems, 0)
    for base, count, out, move in ((0, D2, first_v, moves[0]), (D2, D, second_v, moves[1])):
        done = 0
        while done < count:
            q, off = divmod(skip + base + done, PIECE)
            take = min(count - done, PIECE - off)
            for side in range(2):
                out[done : done + take, side * 128 : side * 128 + 128] = other[
                    q + last * side, off : off + take, :
                ].astype(F32)
            done += take
        move.start()
    for m in moves:
        m.wait()


def run_node_out(other, first, second):
    hbm = pl.BlockSpec(memory_space=pltpu.HBM)
    vm = pl.BlockSpec(memory_space=pltpu.VMEM)
    shapes = [first.shape, second.shape]
    return pl.pallas_call(
        node_out_kernel,
        out_shape=tuple(jax.ShapeDtypeStruct(s, F32) for s in shapes),
        in_specs=[vm, hbm, hbm],
        out_specs=(hbm, hbm),
        input_output_aliases={1: 0, 2: 1},
        scratch_shapes=[pltpu.VMEM((s[0], s[1] // 2), F32) for s in shapes]
        + [pltpu.SemaphoreType.DMA((2,))],
        compiler_params=pltpu.CompilerParams(vmem_limit_bytes=12 * 1024 * 1024),
        cost_estimate=pl.CostEstimate(flops=1_000_000, bytes_accessed=2_000_000, transcendentals=0),
        name="node_out",
    )(other, first, second)


def sum_kernel(pieces, out):
    def add(at):
        total = pieces[0, at, :].astype(F32)
        for p in range(1, pieces.shape[0]):
            total = total + pieces[p, at, :].astype(F32)
        out[at, :] = total.astype(BF)

    step = 32

    @pl.loop(0, PIECE // step)
    def _(i):
        add(pl.ds(pl.multiple_of(i * step, step), step))

    add(slice(PIECE, PIECE + EXTRA))


def run_sum(pieces):
    vm = pl.BlockSpec(memory_space=pltpu.VMEM)
    return pl.pallas_call(
        sum_kernel,
        out_shape=jax.ShapeDtypeStruct(pieces.shape[1:], BF),
        in_specs=[vm],
        out_specs=vm,
        compiler_params=pltpu.CompilerParams(vmem_limit_bytes=4 * 1024 * 1024),
        cost_estimate=pl.CostEstimate(flops=1_000_000, bytes_accessed=2_000_000, transcendentals=0),
        name="sum_pieces",
    )(pieces)


def all_pieces(value, groups):
    return lax.all_to_all(value, ALL, 0, 0, axis_index_groups=groups, tiled=True)


def step(
    nodes,
    edges,
    node_cotangent,
    edge_cotangent,
    senders,
    receivers,
    send_lists,
    edge_first,
    edge_bias,
    edge_second,
    edge_gain,
    node_first,
    node_bias,
    node_second,
    node_gain,
):
    swap = [(0, 1), (1, 0)]
    count = lax.axis_size("space")
    onward = [(i, (i + 1) % count) for i in range(count)]
    backward = [((i + 1) % count, i) for i in range(count)]
    rows = nodes[0]
    lists = send_lists[0]
    D = rows.shape[1]
    H = edge_first.shape[1]
    halo = lists.shape[1]

    bias_row = edge_bias[None]
    first_other = lax.ppermute(edge_first, "hidden", swap)
    second_other = lax.ppermute(edge_second, "hidden", swap)
    bias_other = lax.ppermute(bias_row, "hidden", swap)
    list0, list1 = pick(lists, rows)
    from_prev = lax.ppermute(list1, "space", onward)
    from_next = lax.ppermute(list0, "space", backward)

    ready = run_early(
        (
            senders[None],
            receivers[None],
            rows,
            edge_first,
            bias_row,
            edges[0],
            edge_second,
            edge_gain[None],
            node_first,
            node_bias[None],
            node_second,
            node_gain[None],
            node_cotangent[0],
            edge_cotangent[0],
        ),
        halo,
    )
    grads, gedges, gnodes, back_prev, back_next = run_layer(
        ready,
        (from_prev, from_next, first_other, bias_other, second_other),
    )
    from_next = lax.ppermute(back_prev, "space", backward)
    from_prev = lax.ppermute(back_next, "space", onward)
    pieces = all_pieces(grads, PLANES)
    part = run_sum(pieces)
    other = lax.ppermute(part, ALL, across_z(True))
    part = (part.astype(F32) + other.astype(F32)).astype(BF)
    other = lax.ppermute(part, ALL, across_z(False))
    part = (part.astype(F32) + other.astype(F32)).astype(BF)
    copied = jnp.broadcast_to(part[None], (GROUP, *part.shape))
    full = all_pieces(copied, PLANES)

    split = (3 * D + 2 * H) // PIECE
    mine = full[2 * split :]
    other = lax.ppermute(mine, "hidden", swap)
    (edge_first_grad, edge_second_grad, v0, v1, v2, v3, nfirst, nsecond, grad_nodes) = run_edge_out(
        full, lists, gnodes, from_prev, from_next, D, H
    )
    node_first_grad, node_second_grad = run_node_out(other, nfirst, nsecond)
    return (
        grad_nodes[None],
        gedges[None],
        edge_first_grad,
        v0[0],
        edge_second_grad,
        v1[0],
        node_first_grad,
        v2[0],
        node_second_grad,
        v3[0],
    )


def solution(mesh):
    placed = (
        P("batch", "space", None),
        P("batch", "space", None),
        P("batch", "space", None),
        P("batch", "space", None),
        P("space"),
        P("space"),
        P("space", None, None),
        P(None, "hidden"),
        P("hidden"),
        P("hidden", None),
        P(),
        P(),
        P(),
        P(),
        P(),
    )
    return jax.shard_map(
        step,
        mesh=mesh,
        in_specs=placed,
        out_specs=(
            P("batch", "space", "hidden"),
            P("batch", "space", "hidden"),
            P(None, "hidden"),
            P("hidden"),
            P("hidden", None),
            P(),
            P(),
            P(),
            P(),
            P(),
        ),
        check_vma=False,
    )
```

```python
import jax
import jax.numpy as jnp
from jax import lax
from jax.experimental import pallas as pl
from jax.experimental.pallas import tpu as pltpu
from jax.sharding import PartitionSpec as P


EPS = 1e-05
BF = jnp.bfloat16
F32 = jnp.float32
ALL = ("batch", "space", "hidden")

NX, NY, NZ = 4, 4, 8
GROUP = 32
PIECE = 224
EXTRA = 8


def device_at(x, y, z, core):
    return ((y % 2) * 64 + (x * 2 + y // 2) * 8 + z) * 2 + core


def place_of(device):
    core, rest = device % 2, device // 2
    b, space = rest // 64, rest % 64
    return space // 16, (space // 8) % 2 * 2 + b, space % 8, core


PLANES = [
    [device_at(x, y, 2 * c + k, core) for x in range(NX) for y in range(NY) for k in range(2)]
    for core in range(2)
    for c in range(NZ // 2)
]


def across_z(first):
    pairs = []
    for device in range(2 * NX * NY * NZ):
        x, y, z, core = place_of(device)
        up = (z // 2) % 2 == (0 if first else 1)
        pairs.append((device, device_at(x, y, (z + (2 if up else NZ - 2)) % NZ, core)))
    return pairs


def dot(a, b):
    return jnp.dot(a, b, preferred_element_type=F32)


def dot_tn(a, b):
    return lax.dot_general(a, b, (((0,), (0,)), ((), ())), preferred_element_type=F32)


def dot_nt(a, b):
    return lax.dot_general(a, b, (((1,), (1,)), ((), ())), preferred_element_type=F32)


def silu_parts(pre):
    s = 0.5 * jnp.tanh(0.5 * pre) + 0.5
    return pre * s, s * (1.0 + pre * (1.0 - s))


def row_mean(v):
    return jnp.sum(v, axis=1, keepdims=True) * (1.0 / v.shape[1])


def normalize(z):
    centre = z - row_mean(z)
    scale = lax.rsqrt(row_mean(centre * centre) + EPS)
    return centre * scale, scale


def norm_back(g, normed, scale):
    return scale * (g - row_mean(g) - normed * row_mean(g * normed))


def in_hbm(*arrays):
    return tuple(pltpu.with_memory_space_constraint(a, pltpu.HBM) for a in arrays)


def own_columns(width):
    return pl.multiple_of(lax.axis_index("hidden") * width, width)


def copies(pairs, sems, first):
    return [pltpu.make_async_copy(a, b, sems.at[first + i]) for i, (a, b) in enumerate(pairs)]


def pick_kernel(lists, nodes, first, second, lists_v, nodes_v, sems):
    moves = copies([(lists, lists_v), (nodes, nodes_v)], sems, 0)
    for m in moves:
        m.start()
    for m in moves:
        m.wait()
    N, K = nodes_v.shape[0], lists_v.shape[1]
    for i, out in enumerate((first, second)):
        hot = lax.broadcasted_iota(jnp.int32, (N, K), 0) == lists_v[i : i + 1, :]
        out[...] = dot_tn(hot.astype(F32).astype(BF), nodes_v[...]).astype(BF)


def pick(lists, nodes):
    hbm = pl.BlockSpec(memory_space=pltpu.HBM)
    vm = pl.BlockSpec(memory_space=pltpu.VMEM)
    out = jax.ShapeDtypeStruct((lists.shape[1], nodes.shape[1]), BF)
    return pl.pallas_call(
        pick_kernel,
        out_shape=(out, out),
        in_specs=[hbm, hbm],
        out_specs=(vm, vm),
        scratch_shapes=[
            pltpu.VMEM(lists.shape, jnp.int32),
            pltpu.VMEM(nodes.shape, BF),
            pltpu.SemaphoreType.DMA((2,)),
        ],
        compiler_params=pltpu.CompilerParams(vmem_limit_bytes=4 * 1024 * 1024),
        cost_estimate=pl.CostEstimate(flops=200_000_000, bytes_accessed=400_000, transcendentals=0),
        name="pick",
    )(*in_hbm(lists, nodes))


LOADED = 14


def early_kernel(*refs):
    sources = refs[:LOADED]
    loaded = refs[LOADED : 2 * LOADED - 2]
    hot, part, snd, rcv, sems = refs[2 * LOADED - 2 :]
    moves = copies(list(zip(sources, (snd, rcv) + tuple(loaded))), sems, 0)
    for m in moves:
        m.start()
    nodes, w1m = loaded[0], loaded[1]
    D = nodes.shape[1]
    N, E = nodes.shape[0], snd.shape[1]
    T = hot.shape[0] - N
    for m in moves[0:2]:
        m.wait()
    hot[0:T, :] = (lax.broadcasted_iota(jnp.int32, (T, E), 0) == snd[...]).astype(F32).astype(BF)
    hot[T:, :] = (lax.broadcasted_iota(jnp.int32, (N, E), 0) == rcv[...]).astype(F32).astype(BF)
    for m in moves[2:4]:
        m.wait()
    part[0:N, :] = dot(nodes[...], w1m[D : 2 * D, :]).astype(BF)
    part[N:, :] = dot(nodes[...], w1m[2 * D :, :]).astype(BF)
    for m in moves[4:]:
        m.wait()


def run_early(params, halo):
    N = params[2].shape[0]
    E = params[5].shape[0]
    H = params[3].shape[1]
    hbm = pl.BlockSpec(memory_space=pltpu.HBM)
    vm = pl.BlockSpec(memory_space=pltpu.VMEM)
    outs = [pltpu.VMEM(p.shape, p.dtype) for p in params[2:]]
    outs += [pltpu.VMEM((2 * N + 2 * halo, E), BF), pltpu.VMEM((2 * N, H), BF)]
    return pl.pallas_call(
        early_kernel,
        out_shape=tuple(outs),
        in_specs=[hbm] * LOADED,
        out_specs=(vm,) * len(outs),
        scratch_shapes=[
            pltpu.VMEM(params[0].shape, jnp.int32),
            pltpu.VMEM(params[1].shape, jnp.int32),
            pltpu.SemaphoreType.DMA((LOADED,)),
        ],
        compiler_params=pltpu.CompilerParams(vmem_limit_bytes=8 * 1024 * 1024),
        cost_estimate=pl.CostEstimate(
            flops=1_500_000_000, bytes_accessed=8_000_000, transcendentals=0
        ),
        name="early",
    )(*in_hbm(*params))


def layer_kernel(*refs):
    loaded = refs[:LOADED]
    halo_p, halo_n, w1o, b1o, w2o = refs[LOADED : LOADED + 5]
    grads, gedges, gnodes, to_prev, to_next = refs[LOADED + 5 : LOADED + 10]
    (
        table,
        tw,
        act,
        slope,
        normed,
        scale,
        dz,
        dh,
        msum,
        ndh,
        ndz,
        ndx,
        aggr,
        ginp,
        ge,
        sems,
    ) = refs[LOADED + 10 :]
    nodes, w1m, b1m, edges, w2m, egain, nf, nb, ns, ngain, ncot, ecot, hot, early = loaded
    E, D = edges.shape
    N = nodes.shape[0]
    H = w1m.shape[1]
    T = table.shape[0]
    half = D // 2
    own = own_columns(half)
    side_rows = GROUP * PIECE // 2
    split = (3 * D + 2 * H) // PIECE

    def put(at, value):
        value = value.astype(BF)
        n = value.shape[0]
        done = 0
        while done < n:
            q, off = divmod(at + done, PIECE)
            take = min(n - done, PIECE - off)
            for side in range(2):
                if q < split:
                    piece = q + split * side
                else:
                    piece = 2 * split + (q - split) + (side_rows // PIECE - split) * side
                grads[piece, off : off + take, :] = value[
                    done : done + take, side * 128 : side * 128 + 128
                ]
            done += take

    table[0:N, :] = nodes[...]
    table[N : N + halo_p.shape[0], :] = halo_p[...]
    table[N + halo_p.shape[0] :, :] = halo_n[...]
    tw[0:N, 0:H] = early[0:N, :]
    tw[T:, 0:H] = early[N:, :]
    tw[N:T, 0:H] = dot(table[N:, :], w1m[D : 2 * D, :]).astype(BF)
    tw[0:T, H:] = dot(table[...], w1o[D : 2 * D, :]).astype(BF)
    tw[T:, H:] = dot(nodes[...], w1o[2 * D :, :]).astype(BF)
    bias = jnp.concatenate([b1m[...], b1o[...]], axis=1)
    aggr[...] = jnp.zeros_like(aggr)

    e = edges[...]
    pre = jnp.concatenate([dot(e, w1m[0:D, :]), dot(e, w1o[0:D, :])], axis=1)
    pre = pre + dot_tn(hot[...], tw[...]) + bias
    a, sl = silu_parts(pre)
    a = a.astype(BF)
    act[...] = a
    slope[...] = sl
    z = dot(a[:, 0:H], w2m[...]) + dot(a[:, H:], w2o[...])
    nz, sc = normalize(z)
    normed[...] = nz
    scale[...] = sc
    message = (egain[...] * nz).astype(BF)
    aggr[...] += dot(hot[T:, :], message)

    agg = aggr[...].astype(BF)
    ginp[:, 0:D] = nodes[...]
    ginp[:, D:] = agg
    npre = dot(ginp[...], nf[...]) + nb[...]
    nact, nslope = silu_parts(npre)
    nact = nact.astype(BF)
    nnorm, nscale = normalize(dot(nact, ns[...]))
    up = ncot[...].astype(F32)
    gain_n = jnp.sum(up * nnorm, axis=0, keepdims=True)
    dzn = norm_back(ngain[...] * up, nnorm, nscale).astype(BF)
    ndz[...] = dzn
    dhn = (dot_nt(dzn, ns[...]) * nslope).astype(BF)
    ndh[...] = dhn
    bias_n = jnp.sum(dhn.astype(F32), axis=0, keepdims=True)
    put(3 * D + 2 * H, dot_tn(ginp[...], ndh[:, pl.ds(own, half)]))
    put(5 * D + 2 * H, dot_tn(nact, ndz[:, pl.ds(own, half)]))
    dxn = dot_nt(dhn, nf[...])
    ndx[...] = dxn[:, 0:D]
    ag = dxn[:, D:].astype(BF)
    msum[...] = jnp.zeros_like(msum)

    mg = ecot[...].astype(F32) + dot_tn(hot[T:, :], ag)
    nz = normed[...]
    msum[0:8, :] += jnp.sum((mg * nz).reshape(E // 8, 8, D), axis=0)
    d = norm_back(egain[...] * mg, nz, scale[...]).astype(BF)
    dz[...] = d
    g = jnp.concatenate([dot_nt(d, w2m[...]), dot_nt(d, w2o[...])], axis=1)
    g = (g * slope[...]).astype(BF)
    dh[...] = g
    msum[8:16, :] += jnp.sum(g.astype(F32).reshape(E // 8, 8, D), axis=0)
    part = dot_nt(g[:, 0:H], w1m[pl.ds(own, half), :]) + dot_nt(
        g[:, H:], w1o[pl.ds(own, half), :]
    )
    ge[...] = (ecot[:, pl.ds(own, half)].astype(F32) + part).astype(BF)

    last = pltpu.make_async_copy(ge, gedges, sems.at[0])
    last.start()
    u = dot(hot[...], dh[...]).astype(BF)
    K = halo_p.shape[0]
    at_s = pl.ds(pl.multiple_of(D + own, half), half)
    at_r = pl.ds(pl.multiple_of(2 * D + own, half), half)
    tg = dot_nt(u[0:T, 0:H], w1m[at_s, :]) + dot_nt(u[0:T, H:], w1o[at_s, :])
    rg = dot_nt(u[T:, 0:H], w1m[at_r, :]) + dot_nt(u[T:, H:], w1o[at_r, :])
    to_prev[...] = tg[N : N + K, :].astype(BF)
    to_next[...] = tg[N + K :, :].astype(BF)
    gnodes[...] = ncot[:, pl.ds(own, half)].astype(F32) + ndx[:, pl.ds(own, half)] + tg[0:N] + rg
    second = dot_tn(act[:, 0:H], dz[...])
    put(3 * D, second[:, 0:half])
    put(3 * D + H, second[:, half:])
    put(0, dot_tn(edges[...], dh[:, 0:H]))
    put(D, dot_tn(table[...], u[0:T, 0:H]))
    put(2 * D, dot_tn(nodes[...], u[T:, 0:H]))

    gain_e = jnp.sum(msum[0:8, :], axis=0, keepdims=True)
    bias_e = jnp.sum(msum[8:16, :], axis=0, keepdims=True)[:, 0:H]
    parts = []
    for v in (bias_e, gain_e, bias_n, gain_n):
        parts += [v[:, i : i + 128] for i in range(0, v.shape[1], 128)]
    zero = jnp.zeros((2 * EXTRA - len(parts), 128), F32)
    vec = jnp.concatenate(parts + [zero], axis=0).astype(BF)
    for piece in range(GROUP):
        if piece < 2:
            grads[piece, PIECE:, :] = vec[piece * EXTRA : piece * EXTRA + EXTRA]
        else:
            grads[piece, PIECE:, :] = jnp.zeros((EXTRA, 128), BF)
    last.wait()


LAYER_VMEM = 26 * 1024 * 1024


def run_layer(params, arrived):
    N, D = params[0].shape
    H = params[1].shape[1]
    E = params[3].shape[0]
    T = N + 2 * arrived[0].shape[0]
    hbm = pl.BlockSpec(memory_space=pltpu.HBM)
    vm = pl.BlockSpec(memory_space=pltpu.VMEM)
    return pl.pallas_call(
        layer_kernel,
        out_shape=(
            jax.ShapeDtypeStruct((GROUP, PIECE + EXTRA, 128), BF),
            jax.ShapeDtypeStruct((E, D // 2), BF),
            jax.ShapeDtypeStruct((N, D // 2), F32),
            jax.ShapeDtypeStruct((arrived[0].shape[0], D // 2), BF),
            jax.ShapeDtypeStruct((arrived[0].shape[0], D // 2), BF),
        ),
        in_specs=[vm] * (LOADED + len(arrived)),
        out_specs=(vm, hbm, vm, vm, vm),
        scratch_shapes=[
            pltpu.VMEM((T, D), BF),
            pltpu.VMEM((T + N, 2 * H), BF),
            pltpu.VMEM((E, 2 * H), BF),
            pltpu.VMEM((E, 2 * H), F32),
            pltpu.VMEM((E, D), F32),
            pltpu.VMEM((E, 1), F32),
            pltpu.VMEM((E, D), BF),
            pltpu.VMEM((E, 2 * H), BF),
            pltpu.VMEM((16, D), F32),
            pltpu.VMEM((N, D), BF),
            pltpu.VMEM((N, D), BF),
            pltpu.VMEM((N, D), F32),
            pltpu.VMEM((N, D), F32),
            pltpu.VMEM((N, 2 * D), BF),
            pltpu.VMEM((E, D // 2), BF),
            pltpu.SemaphoreType.DMA((1,)),
        ],
        compiler_params=pltpu.CompilerParams(vmem_limit_bytes=LAYER_VMEM),
        cost_estimate=pl.CostEstimate(
            flops=6_000_000_000, bytes_accessed=12_000_000, transcendentals=1_000_000
        ),
        name="layer",
    )(*params, *arrived)


def edge_out_kernel(
    full,
    lists,
    gnodes,
    back_p,
    back_n,
    first,
    second,
    v0,
    v1,
    v2,
    v3,
    nfirst,
    nsecond,
    gout,
    first_v,
    second_v,
    nfirst_v,
    nsecond_v,
    lists_v,
    sems,
):
    asked = pltpu.make_async_copy(lists, lists_v, sems.at[4])
    asked.start()
    D3, _ = first.shape
    H = second.shape[0]
    half = second.shape[1] // 2
    split = (D3 + 2 * H) // PIECE
    last = GROUP // 2 - split

    def fetch(at, count, put):
        done = 0
        while done < count:
            q, off = divmod(at + done, PIECE)
            take = min(count - done, PIECE - off)
            for side in range(2):
                if q < split:
                    piece = q + split * side
                else:
                    piece = 2 * split + (q - split) + last * side
                put(done, take, side, full[piece, off : off + take, :].astype(F32))
            done += take

    def put_first(done, take, side, value):
        first_v[done : done + take, side * 128 : side * 128 + 128] = value

    fetch(0, D3, put_first)
    D2, D = nfirst.shape
    cols = pl.ds(own_columns(D // 2), D // 2)
    moves = copies(
        [
            (first_v, first),
            (second_v, second),
            (nfirst_v, nfirst.at[:, cols]),
            (nsecond_v, nsecond.at[:, cols]),
        ],
        sems,
        0,
    )
    moves[0].start()
    for part in range(2):

        def put_second(done, take, side, value):
            at = part * half + side * 128
            second_v[done : done + take, at : at + 128] = value

        fetch(D3 + part * H, H, put_second)
    moves[1].start()
    for base, count, target, move in (
        (D3 + 2 * H, D2, nfirst_v, moves[2]),
        (D3 + 2 * H + D2, D, nsecond_v, moves[3]),
    ):

        def put_node(done, take, side, value):
            target[done : done + take, side * 128 : side * 128 + 128] = value

        fetch(base, count, put_node)
        move.start()
    row = 0
    for out in (v0, v1, v2, v3):
        for at in range(0, out.shape[1], 128):
            piece, off = divmod(row, EXTRA)
            tile = full[piece, PIECE:, :].astype(F32)
            out[:, at : at + 128] = tile[off : off + 1, :]
            row += 1
    asked.wait()
    N, K = gnodes.shape[0], back_p.shape[0]
    total = gnodes[...]
    for i, value in enumerate((back_p, back_n)):
        hot = lax.broadcasted_iota(jnp.int32, (N, K), 0) == lists_v[i : i + 1, :]
        total = total + dot(hot.astype(F32).astype(BF), value[...])
    gout[...] = total.astype(BF)
    for m in moves:
        m.wait()


def run_edge_out(full, lists, gnodes, back_p, back_n, D, H):
    hbm = pl.BlockSpec(memory_space=pltpu.HBM)
    vm = pl.BlockSpec(memory_space=pltpu.VMEM)
    shapes = [(3 * D, H), (H, D)]
    outs = shapes + [(1, H), (1, D), (1, D), (1, D), (2 * D, D), (D, D)]
    held = shapes + [(2 * D, D // 2), (D, D // 2)]
    return pl.pallas_call(
        edge_out_kernel,
        out_shape=tuple(jax.ShapeDtypeStruct(s, F32) for s in outs)
        + (jax.ShapeDtypeStruct(gnodes.shape, BF),),
        in_specs=[vm, hbm, vm, vm, vm],
        out_specs=(hbm, hbm, vm, vm, vm, vm, hbm, hbm, vm),
        scratch_shapes=[pltpu.VMEM(s, F32) for s in held]
        + [pltpu.VMEM(lists.shape, jnp.int32), pltpu.SemaphoreType.DMA((5,))],
        compiler_params=pltpu.CompilerParams(vmem_limit_bytes=12 * 1024 * 1024),
        cost_estimate=pl.CostEstimate(flops=1_000_000, bytes_accessed=5_000_000, transcendentals=0),
        name="edge_out",
    )(full, *in_hbm(lists), gnodes, back_p, back_n)


def node_out_kernel(other, first_in, second_in, first, second, first_v, second_v, sems):
    D2, D = first.shape
    half = D // 2
    cols = pl.ds(pl.multiple_of(half - own_columns(half), half), half)
    skip = (3 * D + D2 // 2) % PIECE
    last = other.shape[0] // 2
    moves = copies([(first_v, first.at[:, cols]), (second_v, second.at[:, cols])], sems, 0)
    for base, count, out, move in ((0, D2, first_v, moves[0]), (D2, D, second_v, moves[1])):
        done = 0
        while done < count:
            q, off = divmod(skip + base + done, PIECE)
            take = min(count - done, PIECE - off)
            for side in range(2):
                out[done : done + take, side * 128 : side * 128 + 128] = other[
                    q + last * side, off : off + take, :
                ].astype(F32)
            done += take
        move.start()
    for m in moves:
        m.wait()


def run_node_out(other, first, second):
    hbm = pl.BlockSpec(memory_space=pltpu.HBM)
    vm = pl.BlockSpec(memory_space=pltpu.VMEM)
    shapes = [first.shape, second.shape]
    return pl.pallas_call(
        node_out_kernel,
        out_shape=tuple(jax.ShapeDtypeStruct(s, F32) for s in shapes),
        in_specs=[vm, hbm, hbm],
        out_specs=(hbm, hbm),
        input_output_aliases={1: 0, 2: 1},
        scratch_shapes=[pltpu.VMEM((s[0], s[1] // 2), F32) for s in shapes]
        + [pltpu.SemaphoreType.DMA((2,))],
        compiler_params=pltpu.CompilerParams(vmem_limit_bytes=12 * 1024 * 1024),
        cost_estimate=pl.CostEstimate(flops=1_000_000, bytes_accessed=2_000_000, transcendentals=0),
        name="node_out",
    )(other, first, second)


def sum_kernel(pieces, out):
    def add(at):
        total = pieces[0, at, :].astype(F32)
        for p in range(1, pieces.shape[0]):
            total = total + pieces[p, at, :].astype(F32)
        out[at, :] = total.astype(BF)

    step = 32

    @pl.loop(0, PIECE // step)
    def _(i):
        add(pl.ds(pl.multiple_of(i * step, step), step))

    add(slice(PIECE, PIECE + EXTRA))


def run_sum(pieces):
    vm = pl.BlockSpec(memory_space=pltpu.VMEM)
    return pl.pallas_call(
        sum_kernel,
        out_shape=jax.ShapeDtypeStruct(pieces.shape[1:], BF),
        in_specs=[vm],
        out_specs=vm,
        compiler_params=pltpu.CompilerParams(vmem_limit_bytes=4 * 1024 * 1024),
        cost_estimate=pl.CostEstimate(flops=1_000_000, bytes_accessed=2_000_000, transcendentals=0),
        name="sum_pieces",
    )(pieces)


def spread_kernel(part, other, out):
    total = (part[...].astype(F32) + other[...].astype(F32)).astype(BF)
    for piece in range(out.shape[0]):
        out[piece, :, :] = total


def run_spread(part, other):
    vm = pl.BlockSpec(memory_space=pltpu.VMEM)
    return pl.pallas_call(
        spread_kernel,
        out_shape=jax.ShapeDtypeStruct((GROUP, *part.shape), BF),
        in_specs=[vm, vm],
        out_specs=vm,
        compiler_params=pltpu.CompilerParams(vmem_limit_bytes=4 * 1024 * 1024),
        cost_estimate=pl.CostEstimate(flops=1_000_000, bytes_accessed=2_000_000, transcendentals=0),
        name="spread",
    )(part, other)


def all_pieces(value, groups):
    return lax.all_to_all(value, ALL, 0, 0, axis_index_groups=groups, tiled=True)


def step(
    nodes,
    edges,
    node_cotangent,
    edge_cotangent,
    senders,
    receivers,
    send_lists,
    edge_first,
    edge_bias,
    edge_second,
    edge_gain,
    node_first,
    node_bias,
    node_second,
    node_gain,
):
    swap = [(0, 1), (1, 0)]
    count = lax.axis_size("space")
    onward = [(i, (i + 1) % count) for i in range(count)]
    backward = [((i + 1) % count, i) for i in range(count)]
    rows = nodes[0]
    lists = send_lists[0]
    D = rows.shape[1]
    H = edge_first.shape[1]
    halo = lists.shape[1]

    bias_row = edge_bias[None]
    first_other = lax.ppermute(edge_first, "hidden", swap)
    second_other = lax.ppermute(edge_second, "hidden", swap)
    bias_other = lax.ppermute(bias_row, "hidden", swap)
    list0, list1 = pick(lists, rows)
    from_prev = lax.ppermute(list1, "space", onward)
    from_next = lax.ppermute(list0, "space", backward)

    ready = run_early(
        (
            senders[None],
            receivers[None],
            rows,
            edge_first,
            bias_row,
            edges[0],
            edge_second,
            edge_gain[None],
            node_first,
            node_bias[None],
            node_second,
            node_gain[None],
            node_cotangent[0],
            edge_cotangent[0],
        ),
        halo,
    )
    grads, gedges, gnodes, back_prev, back_next = run_layer(
        ready,
        (from_prev, from_next, first_other, bias_other, second_other),
    )
    from_next = lax.ppermute(back_prev, "space", backward)
    from_prev = lax.ppermute(back_next, "space", onward)
    pieces = all_pieces(grads, PLANES)
    part = run_sum(pieces)
    other = lax.ppermute(part, ALL, across_z(True))
    part = (part.astype(F32) + other.astype(F32)).astype(BF)
    other = lax.ppermute(part, ALL, across_z(False))
    copied = run_spread(part, other)
    full = all_pieces(copied, PLANES)

    split = (3 * D + 2 * H) // PIECE
    mine = full[2 * split :]
    other = lax.ppermute(mine, "hidden", swap)
    (edge_first_grad, edge_second_grad, v0, v1, v2, v3, nfirst, nsecond, grad_nodes) = run_edge_out(
        full, lists, gnodes, from_prev, from_next, D, H
    )
    node_first_grad, node_second_grad = run_node_out(other, nfirst, nsecond)
    return (
        grad_nodes[None],
        gedges[None],
        edge_first_grad,
        v0[0],
        edge_second_grad,
        v1[0],
        node_first_grad,
        v2[0],
        node_second_grad,
        v3[0],
    )


def solution(mesh):
    placed = (
        P("batch", "space", None),
        P("batch", "space", None),
        P("batch", "space", None),
        P("batch", "space", None),
        P("space"),
        P("space"),
        P("space", None, None),
        P(None, "hidden"),
        P("hidden"),
        P("hidden", None),
        P(),
        P(),
        P(),
        P(),
        P(),
    )
    return jax.shard_map(
        step,
        mesh=mesh,
        in_specs=placed,
        out_specs=(
            P("batch", "space", "hidden"),
            P("batch", "space", "hidden"),
            P(None, "hidden"),
            P("hidden"),
            P("hidden", None),
            P(),
            P(),
            P(),
            P(),
            P(),
        ),
        check_vma=False,
    )
```
